32 devices in a mesh: ra: 8 (over y, x, core), dec: 4 (over z).
Axes of the slice: x: 2, y: 2, z: 4, core: 2. Of those that a mesh axis runs over, the one named last changes fastest.
Arguments:
- design: float32 [5, 80, 32, 1024], P(None, None, 'ra', 'dec'), may hold values from -6 to 6
- observed: float32 [80, 32, 1024], P(None, 'ra', 'dec'), may hold values from -6 to 6
- weight: float32 [80, 32, 1024], P(None, 'ra', 'dec'), may hold values from 0.3 to 3
- params: float32 [5, 32, 1024], P(None, 'ra', 'dec'), may hold values from -4 to 4
- offsets: int32 [80, 32, 1024], P(None, 'ra', 'dec'), may hold values from 0 to 8, as said below
- counts: int32 [32, 1024], P('ra', 'dec'), may hold values from 10 to 80, as said below
Outputs:
- new_params: float32 [5, 32, 1024], P(None, 'ra', 'dec')
- reduced_chi: float32 [], replicated
The draws below stay inside these ranges and needn't reach their ends.
Inputs may be any that keep to these rules, and one draw needn't show every extreme that they name: `offsets`: in the first and the last latitude row of cells no offset steps outside the grid in latitude. `counts`: cells near the middle latitude hold more live observations; the two middle latitude rows hold 80.
All inputs are finite; a program needn't handle non-finite values.
Results may differ from the reference program's by a relative error of at most 0.0003.
Values sent between devices are 32-bit elements; how exact they have to be, the bound alone decides.
A program may use at most 64 MiB of HBM per device.

```python
import math
import jax
import jax.numpy as jnp
from jax import lax

NPAR = 5
OBS = 80
NX = 32
NY = 1024


def draw_offsets(key, part):
    key_ra, key_dec = jax.random.split(key)
    step_ra = jax.random.randint(key_ra, (OBS, NX, NY), -1, 2)
    step_dec = jax.random.randint(key_dec, (OBS, NX, NY), -1, 2)
    row = lax.broadcasted_iota(jnp.int32, (OBS, NX, NY), 2)
    step_dec = jnp.where((row == 0) & (step_dec < 0), 0, step_dec)
    step_dec = jnp.where((row == NY - 1) & (step_dec > 0), 0, step_dec)
    return ((step_ra + 1) * 3 + step_dec + 1).astype(jnp.int32)


def draw_counts(key, part):
    lowest = max(1, OBS // 8)
    row = lax.broadcasted_iota(jnp.int32, (NX, NY), 1)
    distance = jnp.abs(2 * row + 1 - NY)
    highest = OBS - (OBS - lowest) * distance // NY
    drawn = jax.random.randint(key, (NX, NY), lowest, highest + 1)
    return jnp.where(distance <= 1, OBS, drawn).astype(jnp.int32)


def levels(key, extent, shards, smallest, largest):
    loudness = 1.0
    for dim, parts in shards:
        draws = jax.random.uniform(jax.random.fold_in(jax.random.fold_in(key, 6), dim), (parts,), jnp.float32, smallest / len(shards), largest / len(shards))
        loudness = loudness * jnp.repeat(jnp.exp(draws), extent[dim] // parts).reshape((-1,) + (1,) * (len(extent) - 1 - dim))
    return loudness


def bell_draw(rng, shape, width, bound, cuts=(), kind=jnp.bfloat16):
    values = jax.random.normal(rng, shape, jnp.float32) * width
    if len(cuts) > 0:
        values = levels(rng, shape, cuts, -0.22, 0.18) * values
    return jnp.clip(values, min=-bound, max=bound).astype(kind)


def setup_inputs(seed: int = 0) -> dict:
    arg_keys = jax.random.split(jax.random.key(seed), 7)
    return {
        "design": bell_draw(arg_keys[0], (NPAR, OBS, NX, NY), 1.0, 6.0, ((2, 8), (3, 4)), jnp.float32),
        "observed": bell_draw(arg_keys[1], (OBS, NX, NY), 1.0, 6.0, ((1, 8), (2, 4)), jnp.float32),
        "weight": jnp.clip(jnp.exp(math.log(3.0) - 2.3025851 * jax.random.uniform(arg_keys[2], (OBS, NX, NY), jnp.float32) ** levels(arg_keys[2], (OBS, NX, NY), ((1, 8), (2, 4)), -0.2, 0.2)), 0.3, 3.0),
        "params": bell_draw(arg_keys[3], (NPAR, NX, NY), 0.5, 4.0, ((1, 8), (2, 4)), jnp.float32),
        "offsets": draw_offsets(jax.random.fold_in(arg_keys[6], 71), 0),
        "counts": draw_counts(jax.random.fold_in(arg_keys[6], 71), 0),
    }


def pair_list():
    pairs = []
    for first in range(5):
        for second in range(first, 5):
            pairs.append((first, second))
    return pairs

def contributions(design, observed, masked_weight, source_params):
    resid = observed
    for comp in range(5):
        resid = resid - design[comp] * source_params[comp][None]
    weighted = masked_weight * resid
    rows = []
    for comp in range(5):
        rows.append(lax.optimization_barrier(jnp.sum(design[comp] * weighted, axis=0)))
    for first, second in pair_list():
        rows.append(lax.optimization_barrier(jnp.sum(masked_weight * design[first] * design[second], axis=0)))
    return (jnp.stack(rows, axis=0), jnp.sum(weighted * resid))

def solve_blocks(stacked):
    rhs = [stacked[comp] for comp in range(5)]
    normal = [[None] * 5 for item in range(5)]
    for place, pair in enumerate(pair_list()):
        first, second = pair
        value = stacked[5 + place]
        if first == second:
            value = value + 1.0
        normal[first][second] = value
        normal[second][first] = value
    lower = [[None] * 5 for item in range(5)]
    for first in range(5):
        for second in range(first + 1):
            running = normal[first][second]
            for inner in range(second):
                running = running - lower[first][inner] * lower[second][inner]
            if first == second:
                lower[first][first] = jnp.sqrt(running)
            else:
                lower[first][second] = running / lower[second][second]
    forward = []
    for first in range(5):
        running = rhs[first]
        for inner in range(first):
            running = running - lower[first][inner] * forward[inner]
        forward.append(running / lower[first][first])
    answer = [None] * 5
    for first in range(4, -1, -1):
        running = forward[first]
        for inner in range(first + 1, 5):
            running = running - lower[inner][first] * answer[inner]
        answer[first] = running / lower[first][first]
    return jnp.stack(answer, axis=0)

def reference(design, observed, weight, params, offsets, counts):
    slots = lax.broadcasted_iota(jnp.int32, observed.shape, 0)
    live = slots < counts[None]
    total = jnp.zeros((20,) + params.shape[1:], jnp.float32)
    chi = jnp.zeros((), jnp.float32)
    for code in range(9):
        step_ra = code // 3 - 1
        step_dec = code % 3 - 1
        source_params = jnp.roll(params, (-step_ra, -step_dec), axis=(1, 2))
        masked_weight = jnp.where(live & (offsets == code), weight, jnp.zeros_like(weight))
        terms, chi_part = contributions(design, observed, masked_weight, source_params)
        total = total + jnp.roll(terms, (step_ra, step_dec), axis=(1, 2))
        chi = chi + chi_part
    new_params = params + solve_blocks(total)
    reduced_chi = chi / jnp.sum(counts).astype(jnp.float32)
    return (new_params, reduced_chi)
```

```python
import functools

import jax
import jax.numpy as jnp
from jax import lax
from jax.experimental import pallas as pl
from jax.experimental.pallas import tpu as pltpu
from jax.sharding import PartitionSpec as P

LANES = 128
PAIRS = [(p, q) for p in range(5) for q in range(p, 5)]
TERMS = 5 + len(PAIRS)
STEPS = (-1, 0, 1)
PASSES = (
    tuple((PAIRS.index(pair), pair) for pair in ((0, 0), (0, 1), (0, 2), (0, 3), (0, 4))),
    tuple((PAIRS.index(pair), pair) for pair in ((1, 1), (1, 2), (1, 3), (1, 4), (2, 2))),
    tuple((PAIRS.index(pair), pair) for pair in ((2, 3), (2, 4), (3, 3), (3, 4), (4, 4))),
)
MESH = pl.DeviceIdType.MESH


def turn(x, shift, axis):
    shift = shift % x.shape[axis]
    return x if shift == 0 else pltpu.roll(x, shift, axis)


def kernel(
    n_ra, n_dec, cells_ra, chunks, unroll,
    d_hbm, o_hbm, w_hbm, p_hbm, off_hbm, cnt_hbm,
    out_ref, chi_ref,
    d_v, o_v, w_v, off_v, p_v, cnt_v, out_ra, out_col, halo_ra, halo_col, near, bins, own,
    send_ra, recv_ra, send_small, recv_small, stat_ra, stat_dec,
    in_sem, one_sem, halo_send, halo_recv, send_sem, recv_sem, stat_send, stat_recv,
):
    slots = d_v.shape[1]
    rows = p_v.shape[1]
    tiles = rows // cells_ra
    size = slots // chunks
    groups = send_ra.shape[1]
    me_ra, me_dec = lax.axis_index("ra"), lax.axis_index("dec")

    def fetches(c):
        part = pl.ds(c * size, size)
        return [
            pltpu.make_async_copy(w_hbm.at[part], w_v.at[part], in_sem.at[1, c]),
            pltpu.make_async_copy(off_hbm.at[part], off_v.at[part], in_sem.at[2, c]),
            pltpu.make_async_copy(d_hbm.at[:, part], d_v.at[:, part], in_sem.at[0, c]),
        ]

    get_counts = pltpu.make_async_copy(cnt_hbm, cnt_v, one_sem.at[0])
    get_params = pltpu.make_async_copy(p_hbm, p_v, one_sem.at[1])
    get_observed = pltpu.make_async_copy(o_hbm, o_v, one_sem.at[2])
    get_counts.start()
    for c in range(chunks):
        for copy in fetches(c):
            copy.start()
        if c == 0:
            get_params.start()
    get_observed.start()

    def device(step_ra, step_dec):
        return (lax.rem(me_ra + step_ra + n_ra, n_ra), lax.rem(me_dec + step_dec + n_dec, n_dec))

    peers = {(a % n_ra, b % n_dec) for a in STEPS for b in STEPS}
    peers |= {(a, 0) for a in range(n_ra)} | {(0, b) for b in range(n_dec)}
    peers = sorted(peers - {(0, 0)})
    barrier = pltpu.get_barrier_semaphore()
    for peer in peers:
        pl.semaphore_signal(barrier, inc=1, device_id=device(*peer), device_id_type=MESH)

    shape = (rows, LANES)
    row = lax.broadcasted_iota(jnp.int32, shape, 0)
    lane = lax.broadcasted_iota(jnp.int32, shape, 1)
    tile = row // cells_ra
    cell = row - tile * cells_ra
    first_tile, last_tile = tile == 0, tile == tiles - 1
    zero = jnp.zeros(shape, jnp.float32)

    def live_weight(s):
        return jnp.where(s < cnt_v[...], w_v[s], 0.0), off_v[s]

    def run(terms, products, begin, count, start):
        def body(t, sums):
            s = begin + 2 * t
            weight, codes = live_weight(s)
            weight_b, codes_b = live_weight(s + 1)
            values, values_b = products(s, weight), products(s + 1, weight_b)
            same = codes == codes_b
            both = [jnp.where(same, x + y, x) for x, y in zip(values, values_b)]
            sums = list(sums)
            for code in range(9):
                hit, hit_b = codes == code, codes_b == code
                for place in range(len(terms)):
                    at = code * len(terms) + place
                    sums[at] = sums[at] + jnp.where(hit, both[place], jnp.where(hit_b, values_b[place], 0.0))
            return tuple(sums)

        step = next(u for u in (unroll, 2, 1) if (count // 2) % u == 0)
        sums = lax.fori_loop(0, count // 2, body, start, unroll=step)
        for code in range(9):
            for place, term in enumerate(terms):
                bins[code * TERMS + term] = sums[code * len(terms) + place]

    def pair_products(group):
        def products(s, weight):
            scaled = {p: weight * d_v[p, s] for p in {pair[0] for _, pair in group}}
            return [scaled[p] * d_v[q, s] for _, (p, q) in group]
        return products

    def pair_terms(group):
        return [5 + place for place, _ in group]

    def observed_products(s, weight):
        scaled = weight * o_v[s]
        return [scaled * d_v[p, s] for p in range(5)]

    none = tuple(zero for _ in range(45))
    terms = pair_terms(PASSES[0])
    for code in range(9):
        for term in terms:
            bins[code * TERMS + term] = zero
    get_counts.wait()

    def chunk(c, carry):
        for copy in fetches(c):
            copy.wait()
        sums = tuple(bins[code * TERMS + term] for code in range(9) for term in terms)
        run(terms, pair_products(PASSES[0]), c * size, size, sums)
        return carry

    lax.fori_loop(0, chunks, chunk, 0)

    get_params.wait()
    columns = [zero, zero]
    packs = [[zero] * halo_ra.shape[1] for _ in range(2)]
    for p in range(5):
        group, spot = divmod(p, cells_ra)
        value = p_v[p]
        columns[0] = jnp.where((lane == p) & first_tile, turn(value, p, 1), columns[0])
        columns[1] = jnp.where((lane == p) & last_tile, turn(value, p + 1, 1), columns[1])
        packs[0][group] = jnp.where(cell == spot, turn(value, spot, 0), packs[0][group])
        packs[1][group] = jnp.where(cell == spot, turn(value, spot - (cells_ra - 1), 0), packs[1][group])
    for side in range(2):
        out_col[side] = columns[side]
        for group in range(halo_ra.shape[1]):
            out_ra[side, group] = packs[side][group]

    @pl.when(me_dec == 0)
    def _():
        for place in (0, 2, 4):
            recv_small[place] = zero

    @pl.when(me_dec == n_dec - 1)
    def _():
        for place in (1, 3, 5):
            recv_small[place] = zero

    def each(copies, arrives, action):
        for way in STEPS:
            chosen = [copy for copy, step in copies if step == way]
            there = me_dec - way if arrives else me_dec + way

            def act(chosen=chosen):
                for copy in chosen:
                    action(copy)

            if way == 0:
                act()
            else:
                pl.when((there >= 0) & (there < n_dec))(act)

    def start(copies):
        each(copies, False, lambda copy: copy.start())

    def sent(copies):
        each(copies, False, lambda copy: copy.wait_send())

    def arrived_all(copies):
        each(copies, True, lambda copy: copy.wait_recv())

    pl.semaphore_wait(barrier, len(peers))
    around = [(0, 1), (1, 1), (-1, 1), (0, -1), (1, -1), (-1, -1)]
    halo_copies = []
    for side, a in enumerate((1, -1)):
        halo_copies.append((pltpu.make_async_remote_copy(
            src_ref=out_ra.at[side], dst_ref=halo_ra.at[side],
            send_sem=halo_send.at[side], recv_sem=halo_recv.at[side],
            device_id=device(-a, 0), device_id_type=MESH,
        ), 0))
    for place, (a, b) in enumerate(around):
        halo_copies.append((pltpu.make_async_remote_copy(
            src_ref=out_col.at[0 if b == 1 else 1], dst_ref=halo_col.at[place],
            send_sem=halo_send.at[2 + place], recv_sem=halo_recv.at[2 + place],
            device_id=device(-a, -b), device_id_type=MESH,
        ), -b))
    start(halo_copies)
    run(pair_terms(PASSES[1]), pair_products(PASSES[1]), 0, slots, none)
    run(pair_terms(PASSES[2]), pair_products(PASSES[2]), 0, slots, none)
    get_observed.wait()
    arrived_all(halo_copies)

    for p in range(5):
        group, spot = divmod(p, cells_ra)
        value = p_v[p]
        column = {}
        for place, (a, b) in enumerate(around):
            column[a, b] = turn(halo_col[place], -1 - p if b == 1 else -p, 1)
        for a in STEPS:
            if a == 0:
                here, after, before = value, column[0, 1], column[0, -1]
            else:
                edge = cells_ra - 1 if a == 1 else 0
                here = jnp.where(
                    cell == edge, turn(halo_ra[0 if a == 1 else 1, group], edge - spot, 0), turn(value, -a, 0))
                after, before = [
                    jnp.where(cell == edge, turn(column[a, b], a * (cells_ra - 1), 0), turn(column[0, b], -a, 0))
                    for b in (1, -1)
                ]
            up = turn(here, 1, 1)
            up_next = turn(jnp.where(last_tile, before, up), cells_ra, 0)
            down = turn(here, -1, 1)
            down_next = turn(jnp.where(first_tile, after, down), -cells_ra, 0)
            code = 3 * (a + 1)
            near[5 * code + p] = jnp.where(lane == 0, up_next, up)
            near[5 * (code + 1) + p] = here
            near[5 * (code + 2) + p] = jnp.where(lane == LANES - 1, down_next, down)

    def squares(s, chi):
        weight, codes = live_weight(s)
        hits = [codes == code for code in range(8)]
        resid = o_v[s]
        for p in range(5):
            source = near[5 * 8 + p]
            for code in range(8):
                source = jnp.where(hits[code], near[5 * code + p], source)
            resid = resid - d_v[p, s] * source
        return chi + weight * resid * resid

    chi = lax.fori_loop(0, slots, squares, zero, unroll=next(u for u in (unroll, 2, 1) if slots % u == 0))
    chi_sum = jnp.sum(chi, axis=0, keepdims=True)
    live_sum = jnp.sum(cnt_v[...], axis=0, keepdims=True).astype(jnp.float32)
    stat_row = lax.broadcasted_iota(jnp.int32, (2, LANES), 0)
    stat_ra[me_ra] = jnp.where(stat_row == 0, chi_sum, live_sum)

    def stat_copies(buffer, me, count, base, target):
        return [
            pltpu.make_async_remote_copy(
                src_ref=buffer.at[me], dst_ref=buffer.at[me],
                send_sem=stat_send.at[base + step - 1], recv_sem=stat_recv.at[base + step - 1],
                device_id=target(step), device_id_type=MESH,
            )
            for step in range(1, count)
        ]

    along_ra = stat_copies(stat_ra, me_ra, n_ra, 0, lambda step: device(step, 0))
    for copy in along_ra:
        copy.start()
    run(list(range(5)), observed_products, 0, slots, none)
    for copy in along_ra:
        copy.wait_recv()
    stat_dec[me_dec] = functools.reduce(lambda x, y: x + y, [stat_ra[k] for k in range(n_ra)])
    along_dec = stat_copies(stat_dec, me_dec, n_dec, n_ra - 1, lambda step: device(0, step))
    for copy in along_dec:
        copy.start()

    def shift_dec(low, mid, high):
        up = turn(high, 1, 1)
        up_next = turn(up, cells_ra, 0)
        down = turn(low, -1, 1)
        down_next = turn(down, -cells_ra, 0)
        kept = (
            mid
            + jnp.where(lane == 0, jnp.where(first_tile, 0.0, up_next), up)
            + jnp.where(lane == LANES - 1, jnp.where(last_tile, 0.0, down_next), down)
        )
        return kept, up_next, down_next

    def pack_dec(packed, place, up_next, down_next):
        high = jnp.where((lane == place) & first_tile, turn(up_next, place, 1), packed[0])
        low = jnp.where((lane == place) & last_tile, turn(down_next, place + 1, 1), packed[1])
        return high, low

    edge = (zero, zero)
    corners = [(zero, zero), (zero, zero)]
    for group in range(groups):
        packed = [[zero] * 3, [zero] * 3]
        for term in range(group * cells_ra, min(TERMS, (group + 1) * cells_ra)):
            spot = term - group * cells_ra
            merged = []
            for at in range(3):
                down, mid, up = [bins[(3 * a + at) * TERMS + term] for a in range(3)]
                merged.append(
                    mid
                    + jnp.where(cell >= 1, turn(up, 1, 0), 0.0)
                    + jnp.where(cell <= cells_ra - 2, turn(down, -1, 0), 0.0)
                )
                packed[0][at] = jnp.where(cell == spot, turn(up, spot - (cells_ra - 1), 0), packed[0][at])
                packed[1][at] = jnp.where(cell == spot, turn(down, spot, 0), packed[1][at])
            kept, up_next, down_next = shift_dec(*merged)
            own[term] = kept
            edge = pack_dec(edge, term, up_next, down_next)
        for side in range(2):
            kept, up_next, down_next = shift_dec(*packed[side])
            send_ra[side, group] = kept
            corners[side] = pack_dec(corners[side], group, up_next, down_next)
    small = [edge[0], edge[1], corners[0][0], corners[0][1], corners[1][0], corners[1][1]]
    small_steps = [(0, 1), (0, -1), (1, 1), (1, -1), (-1, 1), (-1, -1)]
    for place, value in enumerate(small):
        send_small[place] = value

    copies = []
    for side, step in enumerate((1, -1)):
        copies.append((pltpu.make_async_remote_copy(
            src_ref=send_ra.at[side], dst_ref=recv_ra.at[side],
            send_sem=send_sem.at[side], recv_sem=recv_sem.at[side],
            device_id=device(step, 0), device_id_type=MESH,
        ), 0))
    for place, step in enumerate(small_steps):
        copies.append((pltpu.make_async_remote_copy(
            src_ref=send_small.at[place], dst_ref=recv_small.at[place],
            send_sem=send_sem.at[2 + place], recv_sem=recv_sem.at[2 + place],
            device_id=device(*step), device_id_type=MESH,
        ), step[1]))
    start(copies)
    sent(halo_copies)
    for copy in along_ra:
        copy.wait_send()
    for copy in along_dec:
        copy.wait_recv()
    stats = functools.reduce(lambda x, y: x + y, [stat_dec[k] for k in range(n_dec)])
    chi_ref[...] = jnp.full((8,128), jnp.sum(stats[0:1]) / jnp.sum(stats[1:2]))
    for copy in along_dec:
        copy.wait_send()
    arrived_all(copies)

    def unpack_dec(pair, place):
        high = jnp.where((lane == 0) & first_tile, turn(pair[0], -place, 1), 0.0)
        low = jnp.where((lane == LANES - 1) & last_tile, turn(pair[1], -(place + 1), 1), 0.0)
        return high + low

    edge = (recv_small[0], recv_small[1])
    total = []
    for group in range(groups):
        arrived = [
            recv_ra[side, group]
            + unpack_dec((recv_small[2 + 2 * side], recv_small[3 + 2 * side]), group)
            for side in range(2)
        ]
        for term in range(group * cells_ra, min(TERMS, (group + 1) * cells_ra)):
            spot = term - group * cells_ra
            total.append(
                own[term]
                + unpack_dec(edge, term)
                + jnp.where(cell == 0, turn(arrived[0], -spot, 0), 0.0)
                + jnp.where(cell == cells_ra - 1, turn(arrived[1], cells_ra - 1 - spot, 0), 0.0)
            )

    params = [p_v[p] for p in range(5)]
    lower = [[None] * 5 for _ in range(5)]
    inverse = [None] * 5
    forward = []
    for q in range(5):
        for p in range(q, 5):
            running = total[5 + PAIRS.index((q, p))]
            if p == q:
                running = running + 1.0
            for inner in range(q):
                running = running - lower[p][inner] * lower[q][inner]
            if p == q:
                inverse[q] = 1.0 / jnp.sqrt(running)
            else:
                lower[p][q] = running * inverse[q]
    for p in range(5):
        running = total[p] + params[p]
        for inner in range(p):
            running = running - lower[p][inner] * forward[inner]
        forward.append(running * inverse[p])
    answer = [None] * 5
    for p in range(4, -1, -1):
        running = forward[p]
        for inner in range(p + 1, 5):
            running = running - lower[inner][p] * answer[inner]
        answer[p] = running * inverse[p]
        out_ref[p] = answer[p]

    sent(copies)


def per_device(n_ra, n_dec, design, observed, weight, params, offsets, counts):
    slots, cells_ra, cells_dec = observed.shape
    tiles = cells_dec // LANES
    rows = tiles * cells_ra

    def fold(x):
        x = x.reshape(x.shape[:-1] + (tiles, LANES))
        return jnp.swapaxes(x, -3, -2).reshape(x.shape[:-3] + (rows, LANES))

    chunks = next(c for c in (4, 2, 1) if slots % (2 * c) == 0)
    unroll = 2
    groups = -(-TERMS // cells_ra)
    anywhere = pl.BlockSpec(memory_space=pltpu.HBM)
    vmem = pl.BlockSpec(memory_space=pltpu.VMEM)
    new_params, chi = pl.pallas_call(
        functools.partial(kernel, n_ra, n_dec, cells_ra, chunks, unroll),
        out_shape=(
            jax.ShapeDtypeStruct((5, rows, LANES), jnp.float32),
            jax.ShapeDtypeStruct((8,128), jnp.float32),
        ),
        in_specs=[anywhere] * 6,
        out_specs=(vmem, vmem),
        scratch_shapes=[
            pltpu.VMEM((5, slots, rows, LANES), jnp.float32),
            pltpu.VMEM((slots, rows, LANES), jnp.float32),
            pltpu.VMEM((slots, rows, LANES), jnp.float32),
            pltpu.VMEM((slots, rows, LANES), jnp.int32),
            pltpu.VMEM((5, rows, LANES), jnp.float32),
            pltpu.VMEM((rows, LANES), jnp.int32),
            pltpu.VMEM((2, -(-5 // cells_ra), rows, LANES), jnp.float32),
            pltpu.VMEM((2, rows, LANES), jnp.float32),
            pltpu.VMEM((2, -(-5 // cells_ra), rows, LANES), jnp.float32),
            pltpu.VMEM((6, rows, LANES), jnp.float32),
            pltpu.VMEM((45, rows, LANES), jnp.float32),
            pltpu.VMEM((9 * TERMS, rows, LANES), jnp.float32),
            pltpu.VMEM((TERMS, rows, LANES), jnp.float32),
            pltpu.VMEM((2, groups, rows, LANES), jnp.float32),
            pltpu.VMEM((2, groups, rows, LANES), jnp.float32),
            pltpu.VMEM((6, rows, LANES), jnp.float32),
            pltpu.VMEM((6, rows, LANES), jnp.float32),
            pltpu.VMEM((n_ra, 2, LANES), jnp.float32),
            pltpu.VMEM((n_dec, 2, LANES), jnp.float32),
            pltpu.SemaphoreType.DMA((3, chunks)),
            pltpu.SemaphoreType.DMA((3,)),
            pltpu.SemaphoreType.DMA((8,)),
            pltpu.SemaphoreType.DMA((8,)),
            pltpu.SemaphoreType.DMA((8,)),
            pltpu.SemaphoreType.DMA((8,)),
            pltpu.SemaphoreType.DMA((n_ra + n_dec - 2,)),
            pltpu.SemaphoreType.DMA((n_ra + n_dec - 2,)),
        ],
        compiler_params=pltpu.CompilerParams(collective_id=0, has_side_effects=True, vmem_limit_bytes=16*1024*1024),
    )(*[pltpu.with_memory_space_constraint(fold(x), pltpu.HBM) for x in (design, observed, weight, params, offsets, counts)])
    def finish(x_ref, c_ref, out_ref, s_ref):
        out_ref[...] = x_ref[...]
        s_ref[0] = c_ref[0, 0]
    new_params, chi = pl.pallas_call(
        finish,
        out_shape=(
            jax.ShapeDtypeStruct((5, rows, LANES), jnp.float32),
            jax.ShapeDtypeStruct((1,), jnp.float32),
        ),
        in_specs=[vmem, vmem],
        out_specs=(vmem, pl.BlockSpec(memory_space=pltpu.SMEM)),
        compiler_params=pltpu.CompilerParams(vmem_limit_bytes=1024*1024),
    )(new_params, chi)
    new_params = jnp.swapaxes(new_params.reshape(5, tiles, cells_ra, LANES), 1, 2)
    return new_params.reshape(params.shape), chi[0]


def solution(mesh):
    return jax.shard_map(
        functools.partial(per_device, mesh.shape["ra"], mesh.shape["dec"]),
        mesh=mesh,
        in_specs=(
            P(None, None, "ra", "dec"),
            P(None, "ra", "dec"),
            P(None, "ra", "dec"),
            P(None, "ra", "dec"),
            P(None, "ra", "dec"),
            P("ra", "dec"),
        ),
        out_specs=(P(None, "ra", "dec"), P()),
        check_vma=False,
    )
```

```python
import functools

import jax
import jax.numpy as jnp
from jax import lax
from jax.experimental import pallas as pl
from jax.experimental.pallas import tpu as pltpu
from jax.sharding import PartitionSpec as P

LANES = 128
PAIRS = [(p, q) for p in range(5) for q in range(p, 5)]
TERMS = 5 + len(PAIRS)
STEPS = (-1, 0, 1)
GROUPS = (tuple(range(5, 15)), tuple(range(15, TERMS)) + tuple(range(5)))
MESH = pl.DeviceIdType.MESH
QUARTERS = (1, 3)
WIDTH = 4


def turn(x, shift, axis):
    shift = shift % x.shape[axis]
    return x if shift == 0 else pltpu.roll(x, shift, axis)


def kernel(
    n_ra, n_dec, cells_ra, chunks,
    d_hbm, o_hbm, w_hbm, p_hbm, off_hbm, cnt_hbm,
    out_ref, chi_ref,
    data, off_v, p_v, cnt_v, out_ra, out_col, halo_ra, halo_col, near, bins, own,
    send_ra, recv_ra, send_small, recv_small, stat, where_v,
    local_sem, small_sem, send_sem, halo_sem, sums_sem, stat_sem, far_sem,
):
    slots = data.shape[1]
    rows = cnt_v.shape[0]
    tiles = rows // cells_ra
    size = slots // chunks
    groups = send_ra.shape[1]
    me_ra, me_dec = lax.axis_index("ra"), lax.axis_index("dec")
    design, observed, weight = data.at[pl.ds(0, 5)], data.at[5], data.at[6]

    def fetch(c):
        part = pl.ds(c * size, size)
        for source, target in (
            (w_hbm.at[part], weight.at[part]),
            (off_hbm.at[part], off_v.at[part]),
            (d_hbm.at[:, part], design.at[:, part]),
            (o_hbm.at[part], observed.at[part]),
        ):
            pltpu.make_async_copy(source, target, local_sem.at[c]).start()

    def fetched(c):
        part = data.at[:, pl.ds(c * size, size)]
        pltpu.make_async_copy(part, part, local_sem.at[c]).wait()

    pltpu.make_async_copy(cnt_hbm, cnt_v, small_sem.at[0]).start()
    pltpu.make_async_copy(p_hbm, p_v.at[pl.ds(0, 5)], small_sem.at[0]).start()
    fetch(0)

    def device(step_ra, step_dec):
        return (lax.rem(me_ra + step_ra + n_ra, n_ra), lax.rem(me_dec + step_dec + n_dec, n_dec))

    def everyone(action):
        decs = [lax.rem(me_dec + b, n_dec) for b in range(n_dec)]
        for b in range(1, n_dec):
            action((me_ra, decs[b]))

        def group(a, carry):
            there = lax.rem(me_ra + a, n_ra)
            for dec in decs:
                action((there, dec))
            return carry

        lax.fori_loop(1, n_ra, group, 0, unroll=n_ra * n_dec <= 64)

    def signal(sem, target):
        pl.semaphore_signal(sem, inc=1, device_id=target, device_id_type=MESH)

    aside = sorted({1 % n_ra, -1 % n_ra} - {0})
    lines = [(a, 0) for a in range(1, n_ra)] + [(0, b) for b in range(1, n_dec)]
    corners_of = [(me_dec + b, [(a, b) for a in aside]) for b in (1, -1)]
    barrier = pltpu.get_barrier_semaphore()
    greeted = len(lines)
    for dec, peers in corners_of:
        inside = (dec >= 0) & (dec < n_dec)
        greeted = greeted + len(aside) * inside.astype(jnp.int32)

        def greet(peers=peers):
            for peer in peers:
                signal(barrier, device(*peer))

        pl.when(inside)(greet)
    for peer in lines:
        signal(barrier, device(*peer))
    for c in range(1, chunks):
        fetch(c)

    shape = (rows, LANES)
    row = lax.broadcasted_iota(jnp.int32, shape, 0)
    where_v[0] = lax.broadcasted_iota(jnp.int32, shape, 1)
    where_v[1] = row // cells_ra
    where_v[2] = row - where_v[1] * cells_ra

    def position():
        lane, tile, cell = where_v[0], where_v[1], where_v[2]
        return lane, cell, tile == 0, tile == tiles - 1

    zero = jnp.zeros(shape, jnp.float32)

    def clear(at, carry):
        bins[at] = zero
        return carry

    lax.fori_loop(0, 9 * TERMS, clear, 0, unroll=6)
    pltpu.make_async_copy(p_v, p_v, small_sem.at[0]).wait()
    pairs = 2 if size % 4 == 0 else 1

    def products(group, s, scale):
        d = [design[p, s] for p in range(5)]
        scaled = {}

        def by(p):
            if p not in scaled:
                scaled[p] = scale * (observed[s] if p == 5 else d[p])
            return scaled[p]

        return [by(5) * d[term] if term < 5 else by(PAIRS[term - 5][0]) * d[PAIRS[term - 5][1]] for term in group]

    def accumulate(begin, carry):
        def body(t, carry):
            first = begin + 2 * pairs * t
            codes, scales = [], []
            for k in range(2 * pairs):
                scale = jnp.where(first + k < cnt_v[...], weight[first + k], 0.0)
                scales.append(scale)
                codes.append(off_v[first + k])
            same = [codes[2 * k] == codes[2 * k + 1] for k in range(pairs)]
            for group in GROUPS:
                values = [products(group, first + k, scales[k]) for k in range(2 * pairs)]
                both = [
                    [jnp.where(same[k], x + y, x) for x, y in zip(values[2 * k], values[2 * k + 1])]
                    for k in range(pairs)
                ]
                for code in range(9):
                    hits = [c == code for c in codes]
                    for place, term in enumerate(group):
                        total = bins[code * TERMS + term]
                        for k in range(pairs):
                            second = jnp.where(hits[2 * k + 1], values[2 * k + 1][place], 0.0)
                            total = total + jnp.where(hits[2 * k], both[k][place], second)
                        bins[code * TERMS + term] = total
            return carry

        return lax.fori_loop(0, size // (2 * pairs), body, carry)

    def chunk(c, carry):
        fetched(c)
        return accumulate(c * size, carry)

    ends = [-(-chunks * quarter // 4) for quarter in QUARTERS]
    lax.fori_loop(0, ends[0], chunk, 0)

    lane, cell, first_tile, last_tile = position()
    columns = [zero, zero]
    packs = [[zero] * halo_ra.shape[1] for _ in range(2)]
    for p in range(5):
        group, spot = divmod(p, cells_ra)
        value = p_v[p]
        columns[0] = jnp.where((lane == p) & first_tile, turn(value, p, 1), columns[0])
        columns[1] = jnp.where((lane == p) & last_tile, turn(value, p + 1, 1), columns[1])
        packs[0][group] = jnp.where(cell == spot, turn(value, spot, 0), packs[0][group])
        packs[1][group] = jnp.where(cell == spot, turn(value, spot - (cells_ra - 1), 0), packs[1][group])
    for side in range(2):
        out_col[side] = columns[side]
        for group in range(halo_ra.shape[1]):
            out_ra[side, group] = packs[side][group]

    @pl.when(me_dec == 0)
    def _():
        for place in range(0, 3):
            recv_small[place] = zero

    @pl.when(me_dec == n_dec - 1)
    def _():
        for place in range(3, 6):
            recv_small[place] = zero

    def each(arrives, action):
        for way in STEPS:
            there = me_dec - way if arrives else me_dec + way
            if way == 0:
                action(way)
            else:
                pl.when((there >= 0) & (there < n_dec))(functools.partial(action, way))

    def await_bytes(ref, sem):
        pltpu.make_async_copy(ref, ref, sem).wait()

    def remote(source, target, sem, way, step_ra):
        pltpu.make_async_remote_copy(
            src_ref=source, dst_ref=target, send_sem=send_sem.at[way + 1], recv_sem=sem.at[way + 1],
            device_id=device(step_ra, way), device_id_type=MESH,
        ).start()

    pl.semaphore_wait(barrier, greeted)
    around = {1: [(0, 1), (1, 1), (-1, 1)], -1: [(0, -1), (1, -1), (-1, -1)]}
    places = around[1] + around[-1]

    def send_halo(way):
        if way == 0:
            for side, a in enumerate((1, -1)):
                remote(out_ra.at[side], halo_ra.at[side], halo_sem, 0, -a)
        for a, b in around.get(-way, []):
            remote(out_col.at[0 if b == 1 else 1], halo_col.at[places.index((a, b))], halo_sem, way, -a)

    def halo_side(ref, way):
        return ref.at[pl.ds(0 if way == -1 else 3, 3)]

    each(False, send_halo)
    for b in range(1, n_dec):
        signal(far_sem, device(0, b))
    lax.fori_loop(ends[0], ends[1], chunk, 0)
    for c in range(ends[1], chunks):
        fetched(c)
    each(True, lambda way: await_bytes(halo_side(halo_col, way) if way else halo_ra, halo_sem.at[way + 1]))
    around = places
    lane, cell, first_tile, last_tile = position()

    for p in range(5):
        group, spot = divmod(p, cells_ra)
        value = p_v[p]
        column = {}
        for place, (a, b) in enumerate(around):
            column[a, b] = turn(halo_col[place], -1 - p if b == 1 else -p, 1)
        for a in STEPS:
            if a == 0:
                here, after, before = value, column[0, 1], column[0, -1]
            else:
                edge = cells_ra - 1 if a == 1 else 0
                here = jnp.where(
                    cell == edge, turn(halo_ra[0 if a == 1 else 1, group], edge - spot, 0), turn(value, -a, 0))
                after, before = [
                    jnp.where(cell == edge, turn(column[a, b], a * (cells_ra - 1), 0), turn(column[0, b], -a, 0))
                    for b in (1, -1)
                ]
            up = turn(here, 1, 1)
            up_next = turn(jnp.where(last_tile, before, up), cells_ra, 0)
            down = turn(here, -1, 1)
            down_next = turn(jnp.where(first_tile, after, down), -cells_ra, 0)
            code = 3 * (a + 1)
            near[5 * code + p] = jnp.where(lane == 0, up_next, up)
            near[5 * (code + 1) + p] = here
            near[5 * (code + 2) + p] = jnp.where(lane == LANES - 1, down_next, down)

    width = next(u for u in (WIDTH, 2, 1) if slots % u == 0)

    tables = [[near[5 * code + p] for code in range(9)] for p in range(5)]

    def squares(t, chi):
        chosen = []
        for s in range(width):
            codes = off_v[t * width + s]
            low, middle = codes < 3, codes < 6
            codes = codes - jnp.where(low, 0, jnp.where(middle, 3, 6))
            chosen.append((low, middle, codes < 1, codes < 2))
        resids = [observed[t * width + s] for s in range(width)]
        scales = [jnp.where(t * width + s < cnt_v[...], weight[t * width + s], 0.0) for s in range(width)]
        for p in range(5):
            table = tables[p]
            for s, (low, middle, left, centre) in enumerate(chosen):
                row = [jnp.where(low, table[b], jnp.where(middle, table[3 + b], table[6 + b])) for b in range(3)]
                source = jnp.where(left, row[0], jnp.where(centre, row[1], row[2]))
                resids[s] = resids[s] - design[p, t * width + s] * source
        return tuple(x + scales[s] * r * r for s, (x, r) in enumerate(zip(chi, resids)))

    chi = lax.fori_loop(0, slots // width, squares, (zero,) * width)
    chi = functools.reduce(lambda x, y: x + y, chi)
    chi_sum = jnp.sum(chi, axis=0, keepdims=True)
    live_sum = jnp.sum(cnt_v[...], axis=0, keepdims=True).astype(jnp.float32)
    stat_row = lax.broadcasted_iota(jnp.int32, (2, LANES), 0)
    mine = me_ra * n_dec + me_dec
    stat[mine] = jnp.where(stat_row == 0, chi_sum, live_sum)

    def share(target):
        pltpu.make_async_remote_copy(
            src_ref=stat.at[mine], dst_ref=stat.at[mine],
            send_sem=local_sem.at[3], recv_sem=stat_sem.at[0],
            device_id=target, device_id_type=MESH,
        ).start()

    pl.semaphore_wait(far_sem, n_dec - 1)
    everyone(share)

    def shared(sem):
        others = stat.at[pl.ds(0, n_ra * n_dec - 1)]
        pltpu.make_async_copy(others, others, sem).wait()

    lax.fori_loop(ends[1], chunks, lambda c, carry: accumulate(c * size, carry), 0)
    each(False, lambda way: await_bytes(halo_side(halo_col, way) if way else halo_ra, send_sem.at[way + 1]))
    lane, cell, first_tile, last_tile = position()

    def shift_dec(low, mid, high):
        up = turn(high, 1, 1)
        up_next = turn(up, cells_ra, 0)
        down = turn(low, -1, 1)
        down_next = turn(down, -cells_ra, 0)
        kept = (
            mid
            + jnp.where(lane == 0, jnp.where(first_tile, 0.0, up_next), up)
            + jnp.where(lane == LANES - 1, jnp.where(last_tile, 0.0, down_next), down)
        )
        return kept, up_next, down_next

    def pack_dec(packed, place, up_next, down_next):
        high = jnp.where((lane == place) & first_tile, turn(up_next, place, 1), packed[0])
        low = jnp.where((lane == place) & last_tile, turn(down_next, place + 1, 1), packed[1])
        return high, low

    edge = (zero, zero)
    corners = [(zero, zero), (zero, zero)]
    for group in range(groups):
        packed = [[zero] * 3, [zero] * 3]
        for term in range(group * cells_ra, min(TERMS, (group + 1) * cells_ra)):
            spot = term - group * cells_ra
            merged = []
            for at in range(3):
                down, mid, up = [bins[(3 * a + at) * TERMS + term] for a in range(3)]
                merged.append(
                    mid
                    + jnp.where(cell >= 1, turn(up, 1, 0), 0.0)
                    + jnp.where(cell <= cells_ra - 2, turn(down, -1, 0), 0.0)
                )
                packed[0][at] = jnp.where(cell == spot, turn(up, spot - (cells_ra - 1), 0), packed[0][at])
                packed[1][at] = jnp.where(cell == spot, turn(down, spot, 0), packed[1][at])
            kept, up_next, down_next = shift_dec(*merged)
            own[term] = kept
            edge = pack_dec(edge, term, up_next, down_next)
        for side in range(2):
            kept, up_next, down_next = shift_dec(*packed[side])
            send_ra[side, group] = kept
            corners[side] = pack_dec(corners[side], group, up_next, down_next)
    small = {
        (0, 1): edge[0], (0, -1): edge[1],
        (1, 1): corners[0][0], (1, -1): corners[0][1], (-1, 1): corners[1][0], (-1, -1): corners[1][1],
    }
    for place, step in enumerate(places):
        send_small[place] = small[step]

    def send_sums(way):
        if way == 0:
            for side, a in enumerate((1, -1)):
                remote(send_ra.at[side], recv_ra.at[side], sums_sem, 0, a)
        for place, (a, b) in enumerate(places):
            if b == way:
                remote(send_small.at[place], recv_small.at[place], sums_sem, way, a)

    def sums_side(ref, way):
        return ref.at[pl.ds(0 if way == 1 else 3, 3)]

    each(False, send_sums)
    each(True, lambda way: await_bytes(sums_side(recv_small, way) if way else recv_ra, sums_sem.at[way + 1]))
    received = {step: recv_small[place] for place, step in enumerate(places)}

    lane, cell, first_tile, last_tile = position()

    def unpack_dec(pair, place):
        high = jnp.where((lane == 0) & first_tile, turn(pair[0], -place, 1), 0.0)
        low = jnp.where((lane == LANES - 1) & last_tile, turn(pair[1], -(place + 1), 1), 0.0)
        return high + low

    edge = (received[0, 1], received[0, -1])
    total = []
    for group in range(groups):
        arrived = [
            recv_ra[side, group]
            + unpack_dec((received[a, 1], received[a, -1]), group)
            for side, a in enumerate((1, -1))
        ]
        for term in range(group * cells_ra, min(TERMS, (group + 1) * cells_ra)):
            spot = term - group * cells_ra
            total.append(
                own[term]
                + unpack_dec(edge, term)
                + jnp.where(cell == 0, turn(arrived[0], -spot, 0), 0.0)
                + jnp.where(cell == cells_ra - 1, turn(arrived[1], cells_ra - 1 - spot, 0), 0.0)
            )

    params = [p_v[p] for p in range(5)]
    lower = [[None] * 5 for _ in range(5)]
    inverse = [None] * 5
    forward = []
    for q in range(5):
        for p in range(q, 5):
            running = total[5 + PAIRS.index((q, p))]
            if p == q:
                running = running + 1.0
            for inner in range(q):
                running = running - lower[p][inner] * lower[q][inner]
            if p == q:
                inverse[q] = 1.0 / jnp.sqrt(running)
            else:
                lower[p][q] = running * inverse[q]
    for p in range(5):
        running = total[p] + params[p]
        for inner in range(p):
            running = running - lower[p][inner] * forward[inner]
        forward.append(running * inverse[p])
    answer = [None] * 5
    for p in range(4, -1, -1):
        running = forward[p]
        for inner in range(p + 1, 5):
            running = running - lower[inner][p] * answer[inner]
        answer[p] = running * inverse[p]
        out_ref[p] = answer[p]

    shared(stat_sem.at[0])
    stats = functools.reduce(lambda x, y: x + y, [stat[k] for k in range(n_ra * n_dec)])
    chi_ref[...] = jnp.full((8, LANES), jnp.sum(stats[0:1]) / jnp.sum(stats[1:2]))
    shared(local_sem.at[3])
    each(False, lambda way: await_bytes(sums_side(send_small, way) if way else send_ra, send_sem.at[way + 1]))


def per_device(n_ra, n_dec, design, observed, weight, params, offsets, counts):
    slots, cells_ra, cells_dec = observed.shape
    tiles = cells_dec // LANES
    rows = tiles * cells_ra

    def fold(x):
        x = x.reshape(x.shape[:-1] + (tiles, LANES))
        return jnp.swapaxes(x, -3, -2).reshape(x.shape[:-3] + (rows, LANES))

    chunks = next(c for c in (4, 2, 1) if slots % (2 * c) == 0)
    groups = -(-TERMS // cells_ra)
    anywhere = pl.BlockSpec(memory_space=pltpu.HBM)
    vmem = pl.BlockSpec(memory_space=pltpu.VMEM)
    new_params, chi = pl.pallas_call(
        functools.partial(kernel, n_ra, n_dec, cells_ra, chunks),
        out_shape=(
            jax.ShapeDtypeStruct((5, rows, LANES), jnp.float32),
            jax.ShapeDtypeStruct((8,128), jnp.float32),
        ),
        in_specs=[anywhere] * 6,
        out_specs=(vmem, vmem),
        scratch_shapes=[
            pltpu.VMEM((8, slots, rows, LANES), jnp.float32),
            pltpu.VMEM((slots, rows, LANES), jnp.int32),
            pltpu.VMEM((6, rows, LANES), jnp.float32),
            pltpu.VMEM((rows, LANES), jnp.int32),
            pltpu.VMEM((2, -(-5 // cells_ra), rows, LANES), jnp.float32),
            pltpu.VMEM((2, rows, LANES), jnp.float32),
            pltpu.VMEM((2, -(-5 // cells_ra), rows, LANES), jnp.float32),
            pltpu.VMEM((6, rows, LANES), jnp.float32),
            pltpu.VMEM((45, rows, LANES), jnp.float32),
            pltpu.VMEM((9 * TERMS, rows, LANES), jnp.float32),
            pltpu.VMEM((TERMS, rows, LANES), jnp.float32),
            pltpu.VMEM((2, groups, rows, LANES), jnp.float32),
            pltpu.VMEM((2, groups, rows, LANES), jnp.float32),
            pltpu.VMEM((6, rows, LANES), jnp.float32),
            pltpu.VMEM((6, rows, LANES), jnp.float32),
            pltpu.VMEM((n_ra * n_dec, 2, LANES), jnp.float32),
            pltpu.VMEM((3, rows, LANES), jnp.int32),
            pltpu.SemaphoreType.DMA((4,)),
            pltpu.SemaphoreType.DMA((1,)),
            pltpu.SemaphoreType.DMA((3,)),
            pltpu.SemaphoreType.DMA((3,)),
            pltpu.SemaphoreType.DMA((3,)),
            pltpu.SemaphoreType.DMA((1,)),
            pltpu.SemaphoreType.REGULAR,
        ],
        compiler_params=pltpu.CompilerParams(collective_id=0, has_side_effects=True, vmem_limit_bytes=16*1024*1024),
    )(*[pltpu.with_memory_space_constraint(fold(x), pltpu.HBM) for x in (design, observed, weight, params, offsets, counts)])
    def finish(x_ref, c_ref, out_ref, s_ref):
        out_ref[...] = x_ref[...]
        s_ref[0] = c_ref[0, 0]
    new_params, chi = pl.pallas_call(
        finish,
        out_shape=(
            jax.ShapeDtypeStruct((5, rows, LANES), jnp.float32),
            jax.ShapeDtypeStruct((1,), jnp.float32),
        ),
        in_specs=[vmem, vmem],
        out_specs=(vmem, pl.BlockSpec(memory_space=pltpu.SMEM)),
        compiler_params=pltpu.CompilerParams(vmem_limit_bytes=1024*1024),
    )(new_params, chi)
    new_params = jnp.swapaxes(new_params.reshape(5, tiles, cells_ra, LANES), 1, 2)
    return new_params.reshape(params.shape), chi[0]


def solution(mesh):
    return jax.shard_map(
        functools.partial(per_device, mesh.shape["ra"], mesh.shape["dec"]),
        mesh=mesh,
        in_specs=(
            P(None, None, "ra", "dec"),
            P(None, "ra", "dec"),
            P(None, "ra", "dec"),
            P(None, "ra", "dec"),
            P(None, "ra", "dec"),
            P("ra", "dec"),
        ),
        out_specs=(P(None, "ra", "dec"), P()),
        check_vma=False,
    )
```

```python
import functools

import jax
import jax.numpy as jnp
from jax import lax
from jax.experimental import pallas as pl
from jax.experimental.pallas import tpu as pltpu
from jax.sharding import PartitionSpec as P

LANES = 128
PAIRS = [(p, q) for p in range(5) for q in range(p, 5)]
TERMS = 5 + len(PAIRS)
STEPS = (-1, 0, 1)
MESH = pl.DeviceIdType.MESH
EIGHTHS = (0, 7)
RELAYS = (0, 2)
WIDTH = 4


def turn(x, shift, axis):
    shift = shift % x.shape[axis]
    return x if shift == 0 else pltpu.roll(x, shift, axis)


def kernel(
    n_ra, n_dec, cells_ra, chunks,
    d_hbm, o_hbm, w_hbm, p_hbm, off_hbm, cnt_hbm,
    out_ref, chi_ref,
    data, off_v, p_v, cnt_v, out_ra, out_col, halo_ra, halo_col, near, bins, own,
    send_ra, recv_ra, send_small, recv_small, stat, where_v,
    local_sem, small_sem, send_sem, halo_sem, sums_sem, stat_sem, far_sem,
):
    slots = data.shape[1]
    rows = cnt_v.shape[0]
    tiles = rows // cells_ra
    size = slots // chunks
    groups = send_ra.shape[1]
    me_ra, me_dec = lax.axis_index("ra"), lax.axis_index("dec")
    design, observed, weight = data.at[pl.ds(0, 5)], data.at[5], data.at[6]

    def fetch(c):
        part = pl.ds(c * size, size)
        for source, target in (
            (w_hbm.at[part], weight.at[part]),
            (off_hbm.at[part], off_v.at[part]),
            (d_hbm.at[:, part], design.at[:, part]),
            (o_hbm.at[part], observed.at[part]),
        ):
            pltpu.make_async_copy(source, target, local_sem.at[c]).start()

    def fetched(c):
        part = data.at[:, pl.ds(c * size, size)]
        pltpu.make_async_copy(part, part, local_sem.at[c]).wait()

    pltpu.make_async_copy(cnt_hbm, cnt_v, small_sem.at[0]).start()
    pltpu.make_async_copy(p_hbm, p_v.at[pl.ds(0, 5)], small_sem.at[0]).start()
    fetch(0)

    def device(step_ra, step_dec):
        return (lax.rem(me_ra + step_ra + n_ra, n_ra), lax.rem(me_dec + step_dec + n_dec, n_dec))

    def everyone(action):
        decs = [lax.rem(me_dec + b, n_dec) for b in range(n_dec)]
        for b in range(1, n_dec):
            action((me_ra, decs[b]))

        def group(a, carry):
            there = lax.rem(me_ra + a, n_ra)
            for dec in decs:
                action((there, dec))
            return carry

        lax.fori_loop(1, n_ra, group, 0, unroll=n_ra * n_dec <= 64)

    def signal(sem, target):
        pl.semaphore_signal(sem, inc=1, device_id=target, device_id_type=MESH)

    aside = sorted({1 % n_ra, -1 % n_ra} - {0})
    line = [(a, 0) for a in range(1, n_ra)]
    rows_of = [(me_dec + b, [(a, b) for a in (0, *aside)]) for b in (1, -1)]
    barrier = pltpu.get_barrier_semaphore()
    greeted = len(line)
    for dec, peers in rows_of:
        inside = (dec >= 0) & (dec < n_dec)
        greeted = greeted + len(peers) * inside.astype(jnp.int32)

        def greet(peers=peers):
            for peer in peers:
                signal(barrier, device(*peer))

        pl.when(inside)(greet)
    for peer in line:
        signal(barrier, device(*peer))
    for c in range(1, chunks):
        fetch(c)

    shape = (rows, LANES)
    row = lax.broadcasted_iota(jnp.int32, shape, 0)
    where_v[0] = lax.broadcasted_iota(jnp.int32, shape, 1)
    where_v[1] = row // cells_ra
    where_v[2] = row - where_v[1] * cells_ra

    def position():
        lane, tile, cell = where_v[0], where_v[1], where_v[2]
        return lane, cell, tile == 0, tile == tiles - 1

    zero = jnp.zeros(shape, jnp.float32)

    def clear(at, carry):
        bins[at] = zero
        return carry

    lax.fori_loop(0, 9 * TERMS, clear, 0, unroll=6)
    pltpu.make_async_copy(p_v, p_v, small_sem.at[0]).wait()

    def products(s, scale):
        d = [design[p, s] for p in range(5)]
        scaled = [scale * d[p] for p in range(5)]
        return [scaled[p] * observed[s] for p in range(5)] + [scaled[p] * d[q] for p, q in PAIRS]

    def accumulate(begin, count):
        def body(t, carry):
            slot = begin + 2 * t
            codes = [off_v[slot], off_v[slot + 1]]
            scales = [jnp.where(slot + k < cnt_v[...], weight[slot + k], 0.0) for k in range(2)]
            first, second = [products(slot + k, scales[k]) for k in range(2)]
            same = codes[0] == codes[1]
            both = [jnp.where(same, x + y, x) for x, y in zip(first, second)]
            for code in range(9):
                hit, hit_second = codes[0] == code, codes[1] == code
                for term in range(TERMS):
                    value = jnp.where(hit, both[term], jnp.where(hit_second, second[term], 0.0))
                    bins[code * TERMS + term] = bins[code * TERMS + term] + value
            return carry

        lax.fori_loop(0, count // 2, body, 0)

    waited = set()

    def span(begin, end, relays=()):
        pieces = 0
        for c in range(begin // size, -(-end // size)):
            if c not in waited:
                waited.add(c)
                fetched(c)
            first, last = max(begin, c * size), min(end, (c + 1) * size)
            accumulate(first, last - first)
            if pieces in relays and points:
                relay(points.pop(0))
            pieces += 1

    cuts = [2 * (slots * eighth // 16) for eighth in EIGHTHS]
    span(0, cuts[0])

    lane, cell, first_tile, last_tile = position()
    columns = [zero, zero]
    packs = [[zero] * halo_ra.shape[1] for _ in range(2)]
    for p in range(5):
        group, spot = divmod(p, cells_ra)
        value = p_v[p]
        columns[0] = jnp.where((lane == p) & first_tile, turn(value, p, 1), columns[0])
        columns[1] = jnp.where((lane == p) & last_tile, turn(value, p + 1, 1), columns[1])
        packs[0][group] = jnp.where(cell == spot, turn(value, spot, 0), packs[0][group])
        packs[1][group] = jnp.where(cell == spot, turn(value, spot - (cells_ra - 1), 0), packs[1][group])
    for side in range(2):
        out_col[side] = columns[side]
        for group in range(halo_ra.shape[1]):
            out_ra[side, group] = packs[side][group]

    @pl.when(me_dec == 0)
    def _():
        for place in range(0, 3):
            recv_small[place] = zero

    @pl.when(me_dec == n_dec - 1)
    def _():
        for place in range(3, 6):
            recv_small[place] = zero

    def each(arrives, action):
        for way in STEPS:
            there = me_dec - way if arrives else me_dec + way
            if way == 0:
                action(way)
            else:
                pl.when((there >= 0) & (there < n_dec))(functools.partial(action, way))

    def await_bytes(ref, sem):
        pltpu.make_async_copy(ref, ref, sem).wait()

    def edge_rows(b):
        return pl.ds(0 if b == 1 else rows - cells_ra, cells_ra)

    def remote(source, target, sem, way, step_ra):
        pltpu.make_async_remote_copy(
            src_ref=source, dst_ref=target, send_sem=send_sem.at[way + 1], recv_sem=sem.at[way + 1],
            device_id=device(step_ra, way), device_id_type=MESH,
        ).start()

    pl.semaphore_wait(barrier, greeted)
    around = {1: [(0, 1), (1, 1), (-1, 1)], -1: [(0, -1), (1, -1), (-1, -1)]}
    places = around[1] + around[-1]

    def send_halo(way):
        if way == 0:
            for side, a in enumerate((1, -1)):
                remote(out_ra.at[side], halo_ra.at[side], halo_sem, 0, -a)
        for a, b in around.get(-way, []):
            rows_sent = edge_rows(b)
            remote(out_col.at[0 if b == 1 else 1, rows_sent], halo_col.at[places.index((a, b)), rows_sent], halo_sem, way, -a)

    def halo_side(ref, way):
        return ref.at[pl.ds(0 if way == -1 else 3, 3), edge_rows(-way)]

    each(False, send_halo)

    def tell(b):
        there = me_dec + b
        pl.when((there >= 0) & (there < n_dec))(lambda: signal(far_sem.at[max(b, 0)], device(0, b)))

    def hear(b):
        pl.semaphore_wait(far_sem.at[max(b, 0)], 1)
        tell(b)

    def relay(point):
        pl.when(me_dec == 1 + point)(lambda: hear(1))
        pl.when(me_dec == n_dec - 2 - point)(lambda: hear(-1))

    if n_dec > 1:
        pl.when(me_dec == 0)(lambda: tell(1))
        pl.when(me_dec == n_dec - 1)(lambda: tell(-1))
    points = list(range(n_dec - 1))
    span(cuts[0], cuts[1], RELAYS)
    for c in range(chunks):
        if c not in waited:
            waited.add(c)
            fetched(c)
    each(True, lambda way: await_bytes(halo_side(halo_col, way) if way else halo_ra, halo_sem.at[way + 1]))
    around = places
    lane, cell, first_tile, last_tile = position()

    for p in range(5):
        group, spot = divmod(p, cells_ra)
        value = p_v[p]
        column = {}
        for place, (a, b) in enumerate(around):
            column[a, b] = turn(halo_col[place], -1 - p if b == 1 else -p, 1)
        for a in STEPS:
            if a == 0:
                here, after, before = value, column[0, 1], column[0, -1]
            else:
                edge = cells_ra - 1 if a == 1 else 0
                here = jnp.where(
                    cell == edge, turn(halo_ra[0 if a == 1 else 1, group], edge - spot, 0), turn(value, -a, 0))
                after, before = [
                    jnp.where(cell == edge, turn(column[a, b], a * (cells_ra - 1), 0), turn(column[0, b], -a, 0))
                    for b in (1, -1)
                ]
            up = turn(here, 1, 1)
            up_next = turn(jnp.where(last_tile, before, up), cells_ra, 0)
            down = turn(here, -1, 1)
            down_next = turn(jnp.where(first_tile, after, down), -cells_ra, 0)
            code = 3 * (a + 1)
            near[5 * code + p] = jnp.where(lane == 0, up_next, up)
            near[5 * (code + 1) + p] = here
            near[5 * (code + 2) + p] = jnp.where(lane == LANES - 1, down_next, down)

    width = next(u for u in (WIDTH, 2, 1) if slots % u == 0)

    tables = [[near[5 * code + p] for code in range(9)] for p in range(5)]

    def squares(t, chi):
        chosen = []
        for s in range(width):
            codes = off_v[t * width + s]
            low, middle = codes < 3, codes < 6
            codes = codes - jnp.where(low, 0, jnp.where(middle, 3, 6))
            chosen.append((low, middle, codes < 1, codes < 2))
        resids = [observed[t * width + s] for s in range(width)]
        scales = [jnp.where(t * width + s < cnt_v[...], weight[t * width + s], 0.0) for s in range(width)]
        for p in range(5):
            table = tables[p]
            for s, (low, middle, left, centre) in enumerate(chosen):
                row = [jnp.where(low, table[b], jnp.where(middle, table[3 + b], table[6 + b])) for b in range(3)]
                source = jnp.where(left, row[0], jnp.where(centre, row[1], row[2]))
                resids[s] = resids[s] - design[p, t * width + s] * source
        return tuple(x + scales[s] * r * r for s, (x, r) in enumerate(zip(chi, resids)))

    chi = lax.fori_loop(0, slots // width, squares, (zero,) * width)
    chi = functools.reduce(lambda x, y: x + y, chi)
    chi_sum = jnp.sum(chi, axis=0, keepdims=True)
    live_sum = jnp.sum(cnt_v[...], axis=0, keepdims=True).astype(jnp.float32)
    half = lax.broadcasted_iota(jnp.int32, (1, LANES), 1) < LANES // 2
    mine = me_ra * n_dec + me_dec
    folded = jnp.where(half, chi_sum, live_sum) + turn(jnp.where(half, live_sum, chi_sum), LANES // 2, 1)
    stat[mine] = folded

    def share(target):
        pltpu.make_async_remote_copy(
            src_ref=stat.at[mine], dst_ref=stat.at[mine],
            send_sem=local_sem.at[3], recv_sem=stat_sem.at[0],
            device_id=target, device_id_type=MESH,
        ).start()

    while points:
        relay(points.pop(0))
    everyone(share)

    def shared(sem):
        others = stat.at[pl.ds(0, n_ra * n_dec - 1)]
        pltpu.make_async_copy(others, others, sem).wait()

    span(cuts[1], slots)
    each(False, lambda way: await_bytes(halo_side(halo_col, way) if way else halo_ra, send_sem.at[way + 1]))
    lane, cell, first_tile, last_tile = position()

    def shift_dec(low, mid, high):
        up = turn(high, 1, 1)
        up_next = turn(up, cells_ra, 0)
        down = turn(low, -1, 1)
        down_next = turn(down, -cells_ra, 0)
        kept = (
            mid
            + jnp.where(lane == 0, jnp.where(first_tile, 0.0, up_next), up)
            + jnp.where(lane == LANES - 1, jnp.where(last_tile, 0.0, down_next), down)
        )
        return kept, up_next, down_next

    def pack_dec(packed, place, up_next, down_next):
        high = jnp.where((lane == place) & first_tile, turn(up_next, place, 1), packed[0])
        low = jnp.where((lane == place) & last_tile, turn(down_next, place + 1, 1), packed[1])
        return high, low

    edge = (zero, zero)
    corners = [(zero, zero), (zero, zero)]
    for group in range(groups):
        packed = [[zero] * 3, [zero] * 3]
        for term in range(group * cells_ra, min(TERMS, (group + 1) * cells_ra)):
            spot = term - group * cells_ra
            merged = []
            for at in range(3):
                down, mid, up = [bins[(3 * a + at) * TERMS + term] for a in range(3)]
                merged.append(
                    mid
                    + jnp.where(cell >= 1, turn(up, 1, 0), 0.0)
                    + jnp.where(cell <= cells_ra - 2, turn(down, -1, 0), 0.0)
                )
                packed[0][at] = jnp.where(cell == spot, turn(up, spot - (cells_ra - 1), 0), packed[0][at])
                packed[1][at] = jnp.where(cell == spot, turn(down, spot, 0), packed[1][at])
            kept, up_next, down_next = shift_dec(*merged)
            own[term] = kept
            edge = pack_dec(edge, term, up_next, down_next)
        for side in range(2):
            kept, up_next, down_next = shift_dec(*packed[side])
            send_ra[side, group] = kept
            corners[side] = pack_dec(corners[side], group, up_next, down_next)
    small = {
        (0, 1): edge[0], (0, -1): edge[1],
        (1, 1): corners[0][0], (1, -1): corners[0][1], (-1, 1): corners[1][0], (-1, -1): corners[1][1],
    }
    for place, step in enumerate(places):
        send_small[place] = small[step]

    def send_sums(way):
        if way == 0:
            for side, a in enumerate((1, -1)):
                remote(send_ra.at[side], recv_ra.at[side], sums_sem, 0, a)
        for place, (a, b) in enumerate(places):
            if b == way:
                remote(send_small.at[place, edge_rows(b)], recv_small.at[place, edge_rows(b)], sums_sem, way, a)

    def sums_side(ref, way):
        return ref.at[pl.ds(0 if way == 1 else 3, 3), edge_rows(way)]

    each(False, send_sums)
    each(True, lambda way: await_bytes(sums_side(recv_small, way) if way else recv_ra, sums_sem.at[way + 1]))
    received = {step: recv_small[place] for place, step in enumerate(places)}

    lane, cell, first_tile, last_tile = position()

    def unpack_dec(pair, place):
        high = jnp.where((lane == 0) & first_tile, turn(pair[0], -place, 1), 0.0)
        low = jnp.where((lane == LANES - 1) & last_tile, turn(pair[1], -(place + 1), 1), 0.0)
        return high + low

    edge = (received[0, 1], received[0, -1])
    total = []
    for group in range(groups):
        arrived = [
            recv_ra[side, group]
            + unpack_dec((received[a, 1], received[a, -1]), group)
            for side, a in enumerate((1, -1))
        ]
        for term in range(group * cells_ra, min(TERMS, (group + 1) * cells_ra)):
            spot = term - group * cells_ra
            total.append(
                own[term]
                + unpack_dec(edge, term)
                + jnp.where(cell == 0, turn(arrived[0], -spot, 0), 0.0)
                + jnp.where(cell == cells_ra - 1, turn(arrived[1], cells_ra - 1 - spot, 0), 0.0)
            )

    params = [p_v[p] for p in range(5)]
    lower = [[None] * 5 for _ in range(5)]
    inverse = [None] * 5
    forward = []
    for q in range(5):
        for p in range(q, 5):
            running = total[5 + PAIRS.index((q, p))]
            if p == q:
                running = running + 1.0
            for inner in range(q):
                running = running - lower[p][inner] * lower[q][inner]
            if p == q:
                inverse[q] = 1.0 / jnp.sqrt(running)
            else:
                lower[p][q] = running * inverse[q]
    for p in range(5):
        running = total[p] + params[p]
        for inner in range(p):
            running = running - lower[p][inner] * forward[inner]
        forward.append(running * inverse[p])
    answer = [None] * 5
    for p in range(4, -1, -1):
        running = forward[p]
        for inner in range(p + 1, 5):
            running = running - lower[inner][p] * answer[inner]
        answer[p] = running * inverse[p]
        out_ref[p] = answer[p]

    shared(local_sem.at[3])
    each(False, lambda way: await_bytes(sums_side(send_small, way) if way else send_ra, send_sem.at[way + 1]))
    shared(stat_sem.at[0])
    stats = functools.reduce(lambda x, y: x + y, [stat[k] for k in range(n_ra * n_dec)])
    chi_sum = jnp.sum(jnp.where(half, stats, 0.0), axis=1, keepdims=True)
    live_sum = jnp.sum(jnp.where(half, 0.0, stats), axis=1, keepdims=True)
    chi_ref[0:1] = jnp.broadcast_to(chi_sum / live_sum, (1, LANES))


def per_device(n_ra, n_dec, design, observed, weight, params, offsets, counts):
    slots, cells_ra, cells_dec = observed.shape
    tiles = cells_dec // LANES
    rows = tiles * cells_ra

    def fold(x):
        x = x.reshape(x.shape[:-1] + (tiles, LANES))
        return jnp.swapaxes(x, -3, -2).reshape(x.shape[:-3] + (rows, LANES))

    chunks = next(c for c in (4, 2, 1) if slots % (2 * c) == 0)
    groups = -(-TERMS // cells_ra)
    anywhere = pl.BlockSpec(memory_space=pltpu.HBM)
    vmem = pl.BlockSpec(memory_space=pltpu.VMEM)
    new_params, chi = pl.pallas_call(
        functools.partial(kernel, n_ra, n_dec, cells_ra, chunks),
        out_shape=(
            jax.ShapeDtypeStruct((5, rows, LANES), jnp.float32),
            jax.ShapeDtypeStruct((8,128), jnp.float32),
        ),
        in_specs=[anywhere] * 6,
        out_specs=(vmem, vmem),
        scratch_shapes=[
            pltpu.VMEM((8, slots, rows, LANES), jnp.float32),
            pltpu.VMEM((slots, rows, LANES), jnp.int32),
            pltpu.VMEM((6, rows, LANES), jnp.float32),
            pltpu.VMEM((rows, LANES), jnp.int32),
            pltpu.VMEM((2, -(-5 // cells_ra), rows, LANES), jnp.float32),
            pltpu.VMEM((2, rows, LANES), jnp.float32),
            pltpu.VMEM((2, -(-5 // cells_ra), rows, LANES), jnp.float32),
            pltpu.VMEM((6, rows, LANES), jnp.float32),
            pltpu.VMEM((45, rows, LANES), jnp.float32),
            pltpu.VMEM((9 * TERMS, rows, LANES), jnp.float32),
            pltpu.VMEM((TERMS, rows, LANES), jnp.float32),
            pltpu.VMEM((2, groups, rows, LANES), jnp.float32),
            pltpu.VMEM((2, groups, rows, LANES), jnp.float32),
            pltpu.VMEM((6, rows, LANES), jnp.float32),
            pltpu.VMEM((6, rows, LANES), jnp.float32),
            pltpu.VMEM((n_ra * n_dec, 1, LANES), jnp.float32),
            pltpu.VMEM((3, rows, LANES), jnp.int32),
            pltpu.SemaphoreType.DMA((4,)),
            pltpu.SemaphoreType.DMA((1,)),
            pltpu.SemaphoreType.DMA((3,)),
            pltpu.SemaphoreType.DMA((3,)),
            pltpu.SemaphoreType.DMA((3,)),
            pltpu.SemaphoreType.DMA((1,)),
            pltpu.SemaphoreType.REGULAR((2,)),
        ],
        compiler_params=pltpu.CompilerParams(collective_id=0, has_side_effects=True, vmem_limit_bytes=16*1024*1024),
    )(*[pltpu.with_memory_space_constraint(fold(x), pltpu.HBM) for x in (design, observed, weight, params, offsets, counts)])
    def finish(x_ref, c_ref, out_ref, s_ref):
        out_ref[...] = x_ref[...]
        s_ref[0] = c_ref[0, 0]
    new_params, chi = pl.pallas_call(
        finish,
        out_shape=(
            jax.ShapeDtypeStruct((5, rows, LANES), jnp.float32),
            jax.ShapeDtypeStruct((1,), jnp.float32),
        ),
        in_specs=[vmem, vmem],
        out_specs=(vmem, pl.BlockSpec(memory_space=pltpu.SMEM)),
        compiler_params=pltpu.CompilerParams(vmem_limit_bytes=1024*1024),
    )(new_params, chi)
    new_params = jnp.swapaxes(new_params.reshape(5, tiles, cells_ra, LANES), 1, 2)
    return new_params.reshape(params.shape), chi[0]


def solution(mesh):
    return jax.shard_map(
        functools.partial(per_device, mesh.shape["ra"], mesh.shape["dec"]),
        mesh=mesh,
        in_specs=(
            P(None, None, "ra", "dec"),
            P(None, "ra", "dec"),
            P(None, "ra", "dec"),
            P(None, "ra", "dec"),
            P(None, "ra", "dec"),
            P("ra", "dec"),
        ),
        out_specs=(P(None, "ra", "dec"), P()),
        check_vma=False,
    )
```

```python
import functools

import jax
import jax.numpy as jnp
from jax import lax
from jax.experimental import pallas as pl
from jax.experimental.pallas import tpu as pltpu
from jax.sharding import PartitionSpec as P

LANES = 128
PAIRS = [(p, q) for p in range(5) for q in range(p, 5)]
TERMS = 5 + len(PAIRS)
STEPS = (-1, 0, 1)
MESH = pl.DeviceIdType.MESH
PARTS = (0, 35)
RELAYS = (1, 2)
WIDTH = 4


def turn(x, shift, axis):
    shift = shift % x.shape[axis]
    return x if shift == 0 else pltpu.roll(x, shift, axis)


def kernel(
    n_ra, n_dec, cells_ra, chunks,
    d_hbm, o_hbm, w_hbm, p_hbm, off_hbm, cnt_hbm,
    out_ref, chi_ref,
    data, off_v, p_v, cnt_v, out_ra, out_col, halo_ra, halo_col, near, bins, own,
    send_ra, recv_ra, send_small, recv_small, stat, where_v,
    local_sem, small_sem, send_sem, halo_sem, sums_sem, stat_sem, far_sem,
):
    slots = data.shape[1]
    rows = cnt_v.shape[0]
    tiles = rows // cells_ra
    size = slots // chunks
    groups = send_ra.shape[1]
    me_ra, me_dec = lax.axis_index("ra"), lax.axis_index("dec")
    design, observed, weight = data.at[pl.ds(0, 5)], data.at[5], data.at[6]

    def fetch(c):
        part = pl.ds(c * size, size)
        for source, target in (
            (w_hbm.at[part], weight.at[part]),
            (off_hbm.at[part], off_v.at[part]),
            (d_hbm.at[:, part], design.at[:, part]),
            (o_hbm.at[part], observed.at[part]),
        ):
            pltpu.make_async_copy(source, target, local_sem.at[c]).start()

    def fetched(c):
        part = data.at[:, pl.ds(c * size, size)]
        pltpu.make_async_copy(part, part, local_sem.at[c]).wait()

    pltpu.make_async_copy(cnt_hbm, cnt_v, small_sem.at[0]).start()
    pltpu.make_async_copy(p_hbm, p_v.at[pl.ds(0, 5)], small_sem.at[0]).start()
    fetch(0)

    def device(step_ra, step_dec):
        return (lax.rem(me_ra + step_ra + n_ra, n_ra), lax.rem(me_dec + step_dec + n_dec, n_dec))

    def everyone(action):
        decs = [lax.rem(me_dec + b, n_dec) for b in range(n_dec)]
        for b in range(1, n_dec):
            action((me_ra, decs[b]))

        def group(a, carry):
            there = lax.rem(me_ra + a, n_ra)
            for dec in decs:
                action((there, dec))
            return carry

        lax.fori_loop(1, n_ra, group, 0, unroll=n_ra * n_dec <= 64)

    def signal(sem, target):
        pl.semaphore_signal(sem, inc=1, device_id=target, device_id_type=MESH)

    aside = sorted({1 % n_ra, -1 % n_ra} - {0})
    line = [(a, 0) for a in range(1, n_ra)]
    rows_of = [(me_dec + b, [(a, b) for a in (0, *aside)]) for b in (1, -1)]
    barrier = pltpu.get_barrier_semaphore()
    greeted = len(line)
    for dec, peers in rows_of:
        inside = (dec >= 0) & (dec < n_dec)
        greeted = greeted + len(peers) * inside.astype(jnp.int32)

        def greet(peers=peers):
            for peer in peers:
                signal(barrier, device(*peer))

        pl.when(inside)(greet)
    for peer in line:
        signal(barrier, device(*peer))
    for c in range(1, chunks):
        fetch(c)

    shape = (rows, LANES)
    row = lax.broadcasted_iota(jnp.int32, shape, 0)
    where_v[0] = lax.broadcasted_iota(jnp.int32, shape, 1)
    where_v[1] = row // cells_ra
    where_v[2] = row - where_v[1] * cells_ra

    def position():
        lane, tile, cell = where_v[0], where_v[1], where_v[2]
        return lane, cell, tile == 0, tile == tiles - 1

    zero = jnp.zeros(shape, jnp.float32)

    def clear(at, carry):
        bins[at] = zero
        return carry

    lax.fori_loop(0, 9 * TERMS, clear, 0, unroll=6)
    pltpu.make_async_copy(p_v, p_v, small_sem.at[0]).wait()

    def products(s, scale):
        d = [design[p, s] for p in range(5)]
        scaled = [scale * d[p] for p in range(5)]
        return [scaled[p] * observed[s] for p in range(5)] + [scaled[p] * d[q] for p, q in PAIRS]

    def accumulate(begin, count):
        def body(t, carry):
            slot = begin + 2 * t
            codes = [off_v[slot], off_v[slot + 1]]
            scales = [jnp.where(slot + k < cnt_v[...], weight[slot + k], 0.0) for k in range(2)]
            first, second = [products(slot + k, scales[k]) for k in range(2)]
            same = codes[0] == codes[1]
            both = [jnp.where(same, x + y, x) for x, y in zip(first, second)]
            for code in range(9):
                hit, hit_second = codes[0] == code, codes[1] == code
                for term in range(TERMS):
                    value = jnp.where(hit, both[term], jnp.where(hit_second, second[term], 0.0))
                    bins[code * TERMS + term] = bins[code * TERMS + term] + value
            return carry

        lax.fori_loop(0, count // 2, body, 0)

    waited = set()

    def span(begin, end, relays=()):
        pieces = 0
        for c in range(begin // size, -(-end // size)):
            if c not in waited:
                waited.add(c)
                fetched(c)
            first, last = max(begin, c * size), min(end, (c + 1) * size)
            accumulate(first, last - first)
            if pieces in relays and points:
                relay(points.pop(0))
            pieces += 1

    cuts = [2 * (slots * part // 80) for part in PARTS]
    span(0, cuts[0])

    lane, cell, first_tile, last_tile = position()
    columns = [zero, zero]
    packs = [[zero] * halo_ra.shape[1] for _ in range(2)]
    for p in range(5):
        group, spot = divmod(p, cells_ra)
        value = p_v[p]
        columns[0] = jnp.where((lane == p) & first_tile, turn(value, p, 1), columns[0])
        columns[1] = jnp.where((lane == p) & last_tile, turn(value, p + 1, 1), columns[1])
        packs[0][group] = jnp.where(cell == spot, turn(value, spot, 0), packs[0][group])
        packs[1][group] = jnp.where(cell == spot, turn(value, spot - (cells_ra - 1), 0), packs[1][group])
    for side in range(2):
        out_col[side] = columns[side]
        for group in range(halo_ra.shape[1]):
            out_ra[side, group] = packs[side][group]

    @pl.when(me_dec == 0)
    def _():
        for place in range(0, 3):
            recv_small[place] = zero

    @pl.when(me_dec == n_dec - 1)
    def _():
        for place in range(3, 6):
            recv_small[place] = zero

    def each(action):
        for way in STEPS:
            there = me_dec + way
            if way == 0:
                action(way)
            else:
                pl.when((there >= 0) & (there < n_dec))(functools.partial(action, way))

    def await_bytes(ref, sem):
        pltpu.make_async_copy(ref, ref, sem).wait()

    def edge_rows(b):
        return pl.ds(0 if b == 1 else rows - cells_ra, cells_ra)

    def remote(source, target, sem, way, step_ra):
        pltpu.make_async_remote_copy(
            src_ref=source, dst_ref=target, send_sem=send_sem.at[0], recv_sem=sem.at[0],
            device_id=device(step_ra, way), device_id_type=MESH,
        ).start()

    pl.semaphore_wait(barrier, greeted)
    around = {1: [(0, 1), (1, 1), (-1, 1)], -1: [(0, -1), (1, -1), (-1, -1)]}
    places = around[1] + around[-1]

    def send_halo(way):
        if way == 0:
            for side, a in enumerate((1, -1)):
                remote(out_ra.at[side], halo_ra.at[side], halo_sem, 0, -a)
        for a, b in around.get(-way, []):
            rows_sent = edge_rows(b)
            remote(out_col.at[0 if b == 1 else 1, rows_sent], halo_col.at[places.index((a, b)), rows_sent], halo_sem, way, -a)

    def await_all(planes, sem):
        sides = (me_dec > 0).astype(jnp.int32) + (me_dec < n_dec - 1).astype(jnp.int32)
        for count in range(0 if n_dec == 1 else 1, min(n_dec, 3)):
            size_of = bins.at[pl.ds(0, planes * tiles + 3 * count), pl.ds(0, cells_ra)]
            pl.when(sides == count)(lambda size_of=size_of: await_bytes(size_of, sem.at[0]))

    halo_planes, sums_planes = 2 * halo_ra.shape[1], 2 * groups
    each(send_halo)

    def tell(b):
        there = me_dec + b
        pl.when((there >= 0) & (there < n_dec))(lambda: signal(far_sem.at[max(b, 0)], device(0, b)))

    def hear(b):
        pl.semaphore_wait(far_sem.at[max(b, 0)], 1)
        tell(b)

    def relay(point):
        pl.when(me_dec == 1 + point)(lambda: hear(1))
        pl.when(me_dec == n_dec - 2 - point)(lambda: hear(-1))

    if n_dec > 1:
        pl.when(me_dec == 0)(lambda: tell(1))
        pl.when(me_dec == n_dec - 1)(lambda: tell(-1))
    points = list(range(n_dec - 1))
    span(cuts[0], cuts[1], RELAYS)
    for c in range(chunks):
        if c not in waited:
            waited.add(c)
            fetched(c)
    await_all(halo_planes, halo_sem)
    around = places
    lane, cell, first_tile, last_tile = position()

    for p in range(5):
        group, spot = divmod(p, cells_ra)
        value = p_v[p]
        column = {}
        for place, (a, b) in enumerate(around):
            column[a, b] = turn(halo_col[place], -1 - p if b == 1 else -p, 1)
        for a in STEPS:
            if a == 0:
                here, after, before = value, column[0, 1], column[0, -1]
            else:
                edge = cells_ra - 1 if a == 1 else 0
                here = jnp.where(
                    cell == edge, turn(halo_ra[0 if a == 1 else 1, group], edge - spot, 0), turn(value, -a, 0))
                after, before = [
                    jnp.where(cell == edge, turn(column[a, b], a * (cells_ra - 1), 0), turn(column[0, b], -a, 0))
                    for b in (1, -1)
                ]
            up = turn(here, 1, 1)
            up_next = turn(jnp.where(last_tile, before, up), cells_ra, 0)
            down = turn(here, -1, 1)
            down_next = turn(jnp.where(first_tile, after, down), -cells_ra, 0)
            code = 3 * (a + 1)
            near[5 * code + p] = jnp.where(lane == 0, up_next, up)
            near[5 * (code + 1) + p] = here
            near[5 * (code + 2) + p] = jnp.where(lane == LANES - 1, down_next, down)

    width = next(u for u in (WIDTH, 2, 1) if slots % u == 0)

    tables = [[near[5 * code + p] for code in range(9)] for p in range(5)]

    def squares(t, chi):
        chosen = []
        for s in range(width):
            codes = off_v[t * width + s]
            low, middle = codes < 3, codes < 6
            codes = codes - jnp.where(low, 0, jnp.where(middle, 3, 6))
            chosen.append((low, middle, codes < 1, codes < 2))
        resids = [observed[t * width + s] for s in range(width)]
        scales = [jnp.where(t * width + s < cnt_v[...], weight[t * width + s], 0.0) for s in range(width)]
        for p in range(5):
            table = tables[p]
            for s, (low, middle, left, centre) in enumerate(chosen):
                row = [jnp.where(low, table[b], jnp.where(middle, table[3 + b], table[6 + b])) for b in range(3)]
                source = jnp.where(left, row[0], jnp.where(centre, row[1], row[2]))
                resids[s] = resids[s] - design[p, t * width + s] * source
        return tuple(x + scales[s] * r * r for s, (x, r) in enumerate(zip(chi, resids)))

    chi = lax.fori_loop(0, slots // width, squares, (zero,) * width)
    chi = functools.reduce(lambda x, y: x + y, chi)
    chi_sum = jnp.sum(chi, axis=0, keepdims=True)
    live_sum = jnp.sum(cnt_v[...], axis=0, keepdims=True).astype(jnp.float32)
    half = lax.broadcasted_iota(jnp.int32, (1, LANES), 1) < LANES // 2
    mine = me_ra * n_dec + me_dec
    folded = jnp.where(half, chi_sum, live_sum) + turn(jnp.where(half, live_sum, chi_sum), LANES // 2, 1)
    stat[mine] = folded

    def share(target):
        pltpu.make_async_remote_copy(
            src_ref=stat.at[mine], dst_ref=stat.at[mine],
            send_sem=local_sem.at[3], recv_sem=stat_sem.at[0],
            device_id=target, device_id_type=MESH,
        ).start()

    while points:
        relay(points.pop(0))
    everyone(share)

    def shared(sem):
        others = stat.at[pl.ds(0, n_ra * n_dec - 1)]
        pltpu.make_async_copy(others, others, sem).wait()

    span(cuts[1], slots)
    await_all(halo_planes, send_sem)
    lane, cell, first_tile, last_tile = position()

    def shift_dec(low, mid, high):
        up = turn(high, 1, 1)
        up_next = turn(up, cells_ra, 0)
        down = turn(low, -1, 1)
        down_next = turn(down, -cells_ra, 0)
        kept = (
            mid
            + jnp.where(lane == 0, jnp.where(first_tile, 0.0, up_next), up)
            + jnp.where(lane == LANES - 1, jnp.where(last_tile, 0.0, down_next), down)
        )
        return kept, up_next, down_next

    def pack_dec(packed, place, up_next, down_next):
        high = jnp.where((lane == place) & first_tile, turn(up_next, place, 1), packed[0])
        low = jnp.where((lane == place) & last_tile, turn(down_next, place + 1, 1), packed[1])
        return high, low

    edge = (zero, zero)
    corners = [(zero, zero), (zero, zero)]
    for group in range(groups):
        packed = [[zero] * 3, [zero] * 3]
        for term in range(group * cells_ra, min(TERMS, (group + 1) * cells_ra)):
            spot = term - group * cells_ra
            merged = []
            for at in range(3):
                down, mid, up = [bins[(3 * a + at) * TERMS + term] for a in range(3)]
                merged.append(
                    mid
                    + jnp.where(cell >= 1, turn(up, 1, 0), 0.0)
                    + jnp.where(cell <= cells_ra - 2, turn(down, -1, 0), 0.0)
                )
                packed[0][at] = jnp.where(cell == spot, turn(up, spot - (cells_ra - 1), 0), packed[0][at])
                packed[1][at] = jnp.where(cell == spot, turn(down, spot, 0), packed[1][at])
            kept, up_next, down_next = shift_dec(*merged)
            own[term] = kept
            edge = pack_dec(edge, term, up_next, down_next)
        for side in range(2):
            kept, up_next, down_next = shift_dec(*packed[side])
            send_ra[side, group] = kept
            corners[side] = pack_dec(corners[side], group, up_next, down_next)
    small = {
        (0, 1): edge[0], (0, -1): edge[1],
        (1, 1): corners[0][0], (1, -1): corners[0][1], (-1, 1): corners[1][0], (-1, -1): corners[1][1],
    }
    for place, step in enumerate(places):
        send_small[place] = small[step]

    def send_sums(way):
        if way == 0:
            for side, a in enumerate((1, -1)):
                remote(send_ra.at[side], recv_ra.at[side], sums_sem, 0, a)
        for place, (a, b) in enumerate(places):
            if b == way:
                remote(send_small.at[place, edge_rows(b)], recv_small.at[place, edge_rows(b)], sums_sem, way, a)

    each(send_sums)
    await_all(sums_planes, sums_sem)
    received = {step: recv_small[place] for place, step in enumerate(places)}

    lane, cell, first_tile, last_tile = position()

    def unpack_dec(pair, place):
        high = jnp.where((lane == 0) & first_tile, turn(pair[0], -place, 1), 0.0)
        low = jnp.where((lane == LANES - 1) & last_tile, turn(pair[1], -(place + 1), 1), 0.0)
        return high + low

    edge = (received[0, 1], received[0, -1])
    total = []
    for group in range(groups):
        arrived = [
            recv_ra[side, group]
            + unpack_dec((received[a, 1], received[a, -1]), group)
            for side, a in enumerate((1, -1))
        ]
        for term in range(group * cells_ra, min(TERMS, (group + 1) * cells_ra)):
            spot = term - group * cells_ra
            total.append(
                own[term]
                + unpack_dec(edge, term)
                + jnp.where(cell == 0, turn(arrived[0], -spot, 0), 0.0)
                + jnp.where(cell == cells_ra - 1, turn(arrived[1], cells_ra - 1 - spot, 0), 0.0)
            )

    params = [p_v[p] for p in range(5)]
    lower = [[None] * 5 for _ in range(5)]
    inverse = [None] * 5
    forward = []
    for q in range(5):
        for p in range(q, 5):
            running = total[5 + PAIRS.index((q, p))]
            if p == q:
                running = running + 1.0
            for inner in range(q):
                running = running - lower[p][inner] * lower[q][inner]
            if p == q:
                inverse[q] = 1.0 / jnp.sqrt(running)
            else:
                lower[p][q] = running * inverse[q]
    for p in range(5):
        running = total[p] + params[p]
        for inner in range(p):
            running = running - lower[p][inner] * forward[inner]
        forward.append(running * inverse[p])
    answer = [None] * 5
    for p in range(4, -1, -1):
        running = forward[p]
        for inner in range(p + 1, 5):
            running = running - lower[inner][p] * answer[inner]
        answer[p] = running * inverse[p]
        out_ref[p] = answer[p]

    shared(local_sem.at[3])
    await_all(sums_planes, send_sem)
    shared(stat_sem.at[0])
    stats = functools.reduce(lambda x, y: x + y, [stat[k] for k in range(n_ra * n_dec)])
    chi_sum = jnp.sum(jnp.where(half, stats, 0.0), axis=1, keepdims=True)
    live_sum = jnp.sum(jnp.where(half, 0.0, stats), axis=1, keepdims=True)
    chi_ref[0:1] = jnp.broadcast_to(chi_sum / live_sum, (1, LANES))


def per_device(n_ra, n_dec, design, observed, weight, params, offsets, counts):
    slots, cells_ra, cells_dec = observed.shape
    tiles = cells_dec // LANES
    rows = tiles * cells_ra

    def fold(x):
        x = x.reshape(x.shape[:-1] + (tiles, LANES))
        return jnp.swapaxes(x, -3, -2).reshape(x.shape[:-3] + (rows, LANES))

    chunks = next(c for c in (4, 2, 1) if slots % (2 * c) == 0)
    groups = -(-TERMS // cells_ra)
    anywhere = pl.BlockSpec(memory_space=pltpu.HBM)
    vmem = pl.BlockSpec(memory_space=pltpu.VMEM)
    new_params, chi = pl.pallas_call(
        functools.partial(kernel, n_ra, n_dec, cells_ra, chunks),
        out_shape=(
            jax.ShapeDtypeStruct((5, rows, LANES), jnp.float32),
            jax.ShapeDtypeStruct((8,128), jnp.float32),
        ),
        in_specs=[anywhere] * 6,
        out_specs=(vmem, vmem),
        scratch_shapes=[
            pltpu.VMEM((8, slots, rows, LANES), jnp.float32),
            pltpu.VMEM((slots, rows, LANES), jnp.int32),
            pltpu.VMEM((6, rows, LANES), jnp.float32),
            pltpu.VMEM((rows, LANES), jnp.int32),
            pltpu.VMEM((2, -(-5 // cells_ra), rows, LANES), jnp.float32),
            pltpu.VMEM((2, rows, LANES), jnp.float32),
            pltpu.VMEM((2, -(-5 // cells_ra), rows, LANES), jnp.float32),
            pltpu.VMEM((6, rows, LANES), jnp.float32),
            pltpu.VMEM((45, rows, LANES), jnp.float32),
            pltpu.VMEM((9 * TERMS, rows, LANES), jnp.float32),
            pltpu.VMEM((TERMS, rows, LANES), jnp.float32),
            pltpu.VMEM((2, groups, rows, LANES), jnp.float32),
            pltpu.VMEM((2, groups, rows, LANES), jnp.float32),
            pltpu.VMEM((6, rows, LANES), jnp.float32),
            pltpu.VMEM((6, rows, LANES), jnp.float32),
            pltpu.VMEM((n_ra * n_dec, 1, LANES), jnp.float32),
            pltpu.VMEM((3, rows, LANES), jnp.int32),
            pltpu.SemaphoreType.DMA((4,)),
            pltpu.SemaphoreType.DMA((1,)),
            pltpu.SemaphoreType.DMA((1,)),
            pltpu.SemaphoreType.DMA((1,)),
            pltpu.SemaphoreType.DMA((1,)),
            pltpu.SemaphoreType.DMA((1,)),
            pltpu.SemaphoreType.REGULAR((2,)),
        ],
        compiler_params=pltpu.CompilerParams(collective_id=0, has_side_effects=True, vmem_limit_bytes=16*1024*1024),
    )(*[pltpu.with_memory_space_constraint(fold(x), pltpu.HBM) for x in (design, observed, weight, params, offsets, counts)])
    def finish(x_ref, c_ref, out_ref, s_ref):
        out_ref[...] = x_ref[...]
        s_ref[...] = c_ref[0:1, 0:1]
    new_params, chi = pl.pallas_call(
        finish,
        out_shape=(
            jax.ShapeDtypeStruct((5, rows, LANES), jnp.float32),
            jax.ShapeDtypeStruct((1, 1), jnp.float32),
        ),
        in_specs=[vmem, vmem],
        out_specs=(vmem, vmem),
        compiler_params=pltpu.CompilerParams(vmem_limit_bytes=1024*1024),
    )(new_params, chi)
    new_params = jnp.swapaxes(new_params.reshape(5, tiles, cells_ra, LANES), 1, 2)
    return new_params.reshape(params.shape), chi[0, 0]


def solution(mesh):
    return jax.shard_map(
        functools.partial(per_device, mesh.shape["ra"], mesh.shape["dec"]),
        mesh=mesh,
        in_specs=(
            P(None, None, "ra", "dec"),
            P(None, "ra", "dec"),
            P(None, "ra", "dec"),
            P(None, "ra", "dec"),
            P(None, "ra", "dec"),
            P("ra", "dec"),
        ),
        out_specs=(P(None, "ra", "dec"), P()),
        check_vma=False,
    )
```

```python
import functools

import jax
import jax.numpy as jnp
from jax import lax
from jax.experimental import pallas as pl
from jax.experimental.pallas import tpu as pltpu
from jax.sharding import PartitionSpec as P

LANES = 128
PAIRS = [(p, q) for p in range(5) for q in range(p, 5)]
TERMS = 5 + len(PAIRS)
STEPS = (-1, 0, 1)
MESH = pl.DeviceIdType.MESH
PARTS = (0, 35)
RELAYS = (1, 2)
WIDTH = 4


def turn(x, shift, axis):
    shift = shift % x.shape[axis]
    return x if shift == 0 else pltpu.roll(x, shift, axis)


def kernel(
    n_ra, n_dec, cells_ra, chunks,
    d_hbm, o_hbm, w_hbm, p_hbm, off_hbm, cnt_hbm,
    out_ref, chi_ref,
    data, off_v, p_v, cnt_v, out_ra, out_col, halo_ra, halo_col, near, bins, own,
    send_ra, recv_ra, send_small, recv_small, stat, where_v,
    local_sem, small_sem, send_sem, halo_sem, sums_sem, stat_sem, far_sem,
):
    slots = data.shape[1]
    rows = cnt_v.shape[0]
    tiles = rows // cells_ra
    size = slots // chunks
    groups = send_ra.shape[1]
    me_ra, me_dec = lax.axis_index("ra"), lax.axis_index("dec")
    design, observed, weight = data.at[pl.ds(0, 5)], data.at[5], data.at[6]

    def fetch(c):
        part = pl.ds(c * size, size)
        for source, target in (
            (w_hbm.at[part], weight.at[part]),
            (off_hbm.at[part], off_v.at[part]),
            (d_hbm.at[:, part], design.at[:, part]),
            (o_hbm.at[part], observed.at[part]),
        ):
            pltpu.make_async_copy(source, target, local_sem.at[c]).start()

    def fetched(c):
        part = data.at[:, pl.ds(c * size, size)]
        pltpu.make_async_copy(part, part, local_sem.at[c]).wait()

    def device(step_ra, step_dec):
        return (lax.rem(me_ra + step_ra + n_ra, n_ra), lax.rem(me_dec + step_dec + n_dec, n_dec))

    def everyone(action):
        decs = [lax.rem(me_dec + b, n_dec) for b in range(n_dec)]
        for b in range(1, n_dec):
            action((me_ra, decs[b]))

        def group(a, carry):
            there = lax.rem(me_ra + a, n_ra)
            for dec in decs:
                action((there, dec))
            return carry

        lax.fori_loop(1, n_ra, group, 0, unroll=n_ra * n_dec <= 64)

    def signal(sem, target):
        pl.semaphore_signal(sem, inc=1, device_id=target, device_id_type=MESH)

    aside = sorted({1 % n_ra, -1 % n_ra} - {0})
    line = [(a, 0) for a in range(1, n_ra)]
    rows_of = [(me_dec + b, [(a, b) for a in (0, *aside)]) for b in (1, -1)]
    barrier = pltpu.get_barrier_semaphore()
    greeted = len(line)
    for dec, peers in rows_of:
        inside = (dec >= 0) & (dec < n_dec)
        greeted = greeted + len(peers) * inside.astype(jnp.int32)

        def greet(peers=peers):
            for peer in peers:
                signal(barrier, device(*peer))

        pl.when(inside)(greet)
    pltpu.make_async_copy(cnt_hbm, cnt_v, small_sem.at[0]).start()
    pltpu.make_async_copy(p_hbm, p_v.at[pl.ds(0, 5)], small_sem.at[0]).start()
    fetch(0)
    for peer in line:
        signal(barrier, device(*peer))
    for c in range(1, chunks):
        fetch(c)

    shape = (rows, LANES)
    row = lax.broadcasted_iota(jnp.int32, shape, 0)
    where_v[0] = lax.broadcasted_iota(jnp.int32, shape, 1)
    where_v[1] = row // cells_ra
    where_v[2] = row - where_v[1] * cells_ra

    def position():
        lane, tile, cell = where_v[0], where_v[1], where_v[2]
        return lane, cell, tile == 0, tile == tiles - 1

    zero = jnp.zeros(shape, jnp.float32)

    def clear(at, carry):
        bins[at] = zero
        return carry

    lax.fori_loop(0, 9 * TERMS, clear, 0, unroll=6)
    pltpu.make_async_copy(p_v, p_v, small_sem.at[0]).wait()

    def products(s, scale):
        d = [design[p, s] for p in range(5)]
        scaled = [scale * d[p] for p in range(5)]
        return [scaled[p] * observed[s] for p in range(5)] + [scaled[p] * d[q] for p, q in PAIRS]

    def accumulate(begin, count):
        def body(t, carry):
            slot = begin + 2 * t
            codes = [off_v[slot], off_v[slot + 1]]
            scales = [jnp.where(slot + k < cnt_v[...], weight[slot + k], 0.0) for k in range(2)]
            first, second = [products(slot + k, scales[k]) for k in range(2)]
            same = codes[0] == codes[1]
            both = [jnp.where(same, x + y, x) for x, y in zip(first, second)]
            for code in range(9):
                hit, hit_second = codes[0] == code, codes[1] == code
                for term in range(TERMS):
                    value = jnp.where(hit, both[term], jnp.where(hit_second, second[term], 0.0))
                    bins[code * TERMS + term] = bins[code * TERMS + term] + value
            return carry

        lax.fori_loop(0, count // 2, body, 0)

    waited = set()

    def span(begin, end, relays=()):
        pieces = 0
        for c in range(begin // size, -(-end // size)):
            if c not in waited:
                waited.add(c)
                fetched(c)
            first, last = max(begin, c * size), min(end, (c + 1) * size)
            accumulate(first, last - first)
            if pieces in relays and points:
                relay(points.pop(0))
            pieces += 1

    cuts = [2 * (slots * part // 80) for part in PARTS]
    span(0, cuts[0])

    lane, cell, first_tile, last_tile = position()
    columns = [zero, zero]
    packs = [[zero] * halo_ra.shape[1] for _ in range(2)]
    for p in range(5):
        group, spot = divmod(p, cells_ra)
        value = p_v[p]
        columns[0] = jnp.where((lane == p) & first_tile, turn(value, p, 1), columns[0])
        columns[1] = jnp.where((lane == p) & last_tile, turn(value, p + 1, 1), columns[1])
        packs[0][group] = jnp.where(cell == spot, turn(value, spot, 0), packs[0][group])
        packs[1][group] = jnp.where(cell == spot, turn(value, spot - (cells_ra - 1), 0), packs[1][group])
    for side in range(2):
        out_col[side] = columns[side]
        for group in range(halo_ra.shape[1]):
            out_ra[side, group] = packs[side][group]

    @pl.when(me_dec == 0)
    def _():
        for place in range(0, 3):
            recv_small[place] = zero

    @pl.when(me_dec == n_dec - 1)
    def _():
        for place in range(3, 6):
            recv_small[place] = zero

    def each(action):
        for way in STEPS:
            there = me_dec + way
            if way == 0:
                action(way)
            else:
                pl.when((there >= 0) & (there < n_dec))(functools.partial(action, way))

    def await_bytes(ref, sem):
        pltpu.make_async_copy(ref, ref, sem).wait()

    def edge_rows(b):
        return pl.ds(0 if b == 1 else rows - cells_ra, cells_ra)

    def remote(source, target, sem, way, step_ra):
        pltpu.make_async_remote_copy(
            src_ref=source, dst_ref=target, send_sem=send_sem.at[0], recv_sem=sem.at[0],
            device_id=device(step_ra, way), device_id_type=MESH,
        ).start()

    pl.semaphore_wait(barrier, greeted)
    around = {1: [(0, 1), (1, 1), (-1, 1)], -1: [(0, -1), (1, -1), (-1, -1)]}
    places = around[1] + around[-1]

    def send_halo(way):
        if way == 0:
            for side, a in enumerate((1, -1)):
                remote(out_ra.at[side], halo_ra.at[side], halo_sem, 0, -a)
        for a, b in around.get(-way, []):
            rows_sent = edge_rows(b)
            remote(out_col.at[0 if b == 1 else 1, rows_sent], halo_col.at[places.index((a, b)), rows_sent], halo_sem, way, -a)

    def await_all(planes, sem):
        sides = (me_dec > 0).astype(jnp.int32) + (me_dec < n_dec - 1).astype(jnp.int32)
        for count in range(0 if n_dec == 1 else 1, min(n_dec, 3)):
            size_of = bins.at[pl.ds(0, planes * tiles + 3 * count), pl.ds(0, cells_ra)]
            pl.when(sides == count)(lambda size_of=size_of: await_bytes(size_of, sem.at[0]))

    halo_planes, sums_planes = 2 * halo_ra.shape[1], 2 * groups
    each(send_halo)

    def tell(b):
        there = me_dec + b
        pl.when((there >= 0) & (there < n_dec))(lambda: signal(far_sem.at[max(b, 0)], device(0, b)))

    def hear(b):
        pl.semaphore_wait(far_sem.at[max(b, 0)], 1)
        tell(b)

    def relay(point):
        pl.when(me_dec == 1 + point)(lambda: hear(1))
        pl.when(me_dec == n_dec - 2 - point)(lambda: hear(-1))

    if n_dec > 1:
        pl.when(me_dec == 0)(lambda: tell(1))
        pl.when(me_dec == n_dec - 1)(lambda: tell(-1))
    points = list(range(n_dec - 1))
    span(cuts[0], cuts[1], RELAYS)
    for c in range(chunks):
        if c not in waited:
            waited.add(c)
            fetched(c)
    await_all(halo_planes, halo_sem)
    around = places
    lane, cell, first_tile, last_tile = position()

    for p in range(5):
        group, spot = divmod(p, cells_ra)
        value = p_v[p]
        column = {}
        for place, (a, b) in enumerate(around):
            column[a, b] = turn(halo_col[place], -1 - p if b == 1 else -p, 1)
        for a in STEPS:
            if a == 0:
                here, after, before = value, column[0, 1], column[0, -1]
            else:
                edge = cells_ra - 1 if a == 1 else 0
                here = jnp.where(
                    cell == edge, turn(halo_ra[0 if a == 1 else 1, group], edge - spot, 0), turn(value, -a, 0))
                after, before = [
                    jnp.where(cell == edge, turn(column[a, b], a * (cells_ra - 1), 0), turn(column[0, b], -a, 0))
                    for b in (1, -1)
                ]
            up = turn(here, 1, 1)
            up_next = turn(jnp.where(last_tile, before, up), cells_ra, 0)
            down = turn(here, -1, 1)
            down_next = turn(jnp.where(first_tile, after, down), -cells_ra, 0)
            code = 3 * (a + 1)
            near[5 * code + p] = jnp.where(lane == 0, up_next, up)
            near[5 * (code + 1) + p] = here
            near[5 * (code + 2) + p] = jnp.where(lane == LANES - 1, down_next, down)

    width = next(u for u in (WIDTH, 2, 1) if slots % u == 0)

    tables = [[near[5 * code + p] for code in range(9)] for p in range(5)]

    def squares(t, chi):
        chosen = []
        for s in range(width):
            codes = off_v[t * width + s]
            low, middle = codes < 3, codes < 6
            codes = codes - jnp.where(low, 0, jnp.where(middle, 3, 6))
            chosen.append((low, middle, codes < 1, codes < 2))
        resids = [observed[t * width + s] for s in range(width)]
        scales = [jnp.where(t * width + s < cnt_v[...], weight[t * width + s], 0.0) for s in range(width)]
        for p in range(5):
            table = tables[p]
            for s, (low, middle, left, centre) in enumerate(chosen):
                row = [jnp.where(low, table[b], jnp.where(middle, table[3 + b], table[6 + b])) for b in range(3)]
                source = jnp.where(left, row[0], jnp.where(centre, row[1], row[2]))
                resids[s] = resids[s] - design[p, t * width + s] * source
        return tuple(x + scales[s] * r * r for s, (x, r) in enumerate(zip(chi, resids)))

    chi = lax.fori_loop(0, slots // width, squares, (zero,) * width)
    chi = functools.reduce(lambda x, y: x + y, chi)
    chi_sum = jnp.sum(chi, axis=0, keepdims=True)
    live_sum = jnp.sum(cnt_v[...], axis=0, keepdims=True).astype(jnp.float32)
    half = lax.broadcasted_iota(jnp.int32, (1, LANES), 1) < LANES // 2
    mine = me_ra * n_dec + me_dec
    folded = jnp.where(half, chi_sum, live_sum) + turn(jnp.where(half, live_sum, chi_sum), LANES // 2, 1)
    stat[mine] = folded

    def share(target):
        pltpu.make_async_remote_copy(
            src_ref=stat.at[mine], dst_ref=stat.at[mine],
            send_sem=local_sem.at[3], recv_sem=stat_sem.at[0],
            device_id=target, device_id_type=MESH,
        ).start()

    while points:
        relay(points.pop(0))
    everyone(share)

    def shared(sem):
        others = stat.at[pl.ds(0, n_ra * n_dec - 1)]
        pltpu.make_async_copy(others, others, sem).wait()

    span(cuts[1], slots)
    await_all(halo_planes, send_sem)
    lane, cell, first_tile, last_tile = position()

    def shift_dec(low, mid, high):
        up = turn(high, 1, 1)
        up_next = turn(up, cells_ra, 0)
        down = turn(low, -1, 1)
        down_next = turn(down, -cells_ra, 0)
        kept = (
            mid
            + jnp.where(lane == 0, jnp.where(first_tile, 0.0, up_next), up)
            + jnp.where(lane == LANES - 1, jnp.where(last_tile, 0.0, down_next), down)
        )
        return kept, up_next, down_next

    def pack_dec(packed, place, up_next, down_next):
        high = jnp.where((lane == place) & first_tile, turn(up_next, place, 1), packed[0])
        low = jnp.where((lane == place) & last_tile, turn(down_next, place + 1, 1), packed[1])
        return high, low

    edge = (zero, zero)
    corners = [(zero, zero), (zero, zero)]
    for group in range(groups):
        packed = [[zero] * 3, [zero] * 3]
        for term in range(group * cells_ra, min(TERMS, (group + 1) * cells_ra)):
            spot = term - group * cells_ra
            merged = []
            for at in range(3):
                down, mid, up = [bins[(3 * a + at) * TERMS + term] for a in range(3)]
                merged.append(
                    mid
                    + jnp.where(cell >= 1, turn(up, 1, 0), 0.0)
                    + jnp.where(cell <= cells_ra - 2, turn(down, -1, 0), 0.0)
                )
                packed[0][at] = jnp.where(cell == spot, turn(up, spot - (cells_ra - 1), 0), packed[0][at])
                packed[1][at] = jnp.where(cell == spot, turn(down, spot, 0), packed[1][at])
            kept, up_next, down_next = shift_dec(*merged)
            own[term] = kept
            edge = pack_dec(edge, term, up_next, down_next)
        for side in range(2):
            kept, up_next, down_next = shift_dec(*packed[side])
            send_ra[side, group] = kept
            corners[side] = pack_dec(corners[side], group, up_next, down_next)
    small = {
        (0, 1): edge[0], (0, -1): edge[1],
        (1, 1): corners[0][0], (1, -1): corners[0][1], (-1, 1): corners[1][0], (-1, -1): corners[1][1],
    }
    for place, step in enumerate(places):
        send_small[place] = small[step]

    def send_sums(way):
        if way == 0:
            for side, a in enumerate((1, -1)):
                remote(send_ra.at[side], recv_ra.at[side], sums_sem, 0, a)
        for place, (a, b) in enumerate(places):
            if b == way:
                remote(send_small.at[place, edge_rows(b)], recv_small.at[place, edge_rows(b)], sums_sem, way, a)

    each(send_sums)
    await_all(sums_planes, sums_sem)
    received = {step: recv_small[place] for place, step in enumerate(places)}

    lane, cell, first_tile, last_tile = position()

    def unpack_dec(pair, place):
        high = jnp.where((lane == 0) & first_tile, turn(pair[0], -place, 1), 0.0)
        low = jnp.where((lane == LANES - 1) & last_tile, turn(pair[1], -(place + 1), 1), 0.0)
        return high + low

    edge = (received[0, 1], received[0, -1])
    total = []
    for group in range(groups):
        arrived = [
            recv_ra[side, group]
            + unpack_dec((received[a, 1], received[a, -1]), group)
            for side, a in enumerate((1, -1))
        ]
        for term in range(group * cells_ra, min(TERMS, (group + 1) * cells_ra)):
            spot = term - group * cells_ra
            total.append(
                own[term]
                + unpack_dec(edge, term)
                + jnp.where(cell == 0, turn(arrived[0], -spot, 0), 0.0)
                + jnp.where(cell == cells_ra - 1, turn(arrived[1], cells_ra - 1 - spot, 0), 0.0)
            )

    params = [p_v[p] for p in range(5)]
    lower = [[None] * 5 for _ in range(5)]
    inverse = [None] * 5
    forward = []
    for q in range(5):
        for p in range(q, 5):
            running = total[5 + PAIRS.index((q, p))]
            if p == q:
                running = running + 1.0
            for inner in range(q):
                running = running - lower[p][inner] * lower[q][inner]
            if p == q:
                inverse[q] = 1.0 / jnp.sqrt(running)
            else:
                lower[p][q] = running * inverse[q]
    for p in range(5):
        running = total[p] + params[p]
        for inner in range(p):
            running = running - lower[p][inner] * forward[inner]
        forward.append(running * inverse[p])
    answer = [None] * 5
    for p in range(4, -1, -1):
        running = forward[p]
        for inner in range(p + 1, 5):
            running = running - lower[inner][p] * answer[inner]
        answer[p] = running * inverse[p]
        out_ref[p] = answer[p]

    shared(local_sem.at[3])
    await_all(sums_planes, send_sem)
    shared(stat_sem.at[0])
    stats = functools.reduce(lambda x, y: x + y, [stat[k] for k in range(n_ra * n_dec)])
    chi_sum = jnp.sum(jnp.where(half, stats, 0.0), axis=1, keepdims=True)
    live_sum = jnp.sum(jnp.where(half, 0.0, stats), axis=1, keepdims=True)
    chi_ref[0:1] = jnp.broadcast_to(chi_sum / live_sum, (1, LANES))


def per_device(n_ra, n_dec, design, observed, weight, params, offsets, counts):
    slots, cells_ra, cells_dec = observed.shape
    tiles = cells_dec // LANES
    rows = tiles * cells_ra

    def fold(x):
        x = x.reshape(x.shape[:-1] + (tiles, LANES))
        return jnp.swapaxes(x, -3, -2).reshape(x.shape[:-3] + (rows, LANES))

    chunks = next(c for c in (4, 2, 1) if slots % (2 * c) == 0)
    groups = -(-TERMS // cells_ra)
    anywhere = pl.BlockSpec(memory_space=pltpu.HBM)
    vmem = pl.BlockSpec(memory_space=pltpu.VMEM)
    new_params, chi = pl.pallas_call(
        functools.partial(kernel, n_ra, n_dec, cells_ra, chunks),
        out_shape=(
            jax.ShapeDtypeStruct((5, rows, LANES), jnp.float32),
            jax.ShapeDtypeStruct((8,128), jnp.float32),
        ),
        in_specs=[anywhere] * 6,
        out_specs=(vmem, vmem),
        scratch_shapes=[
            pltpu.VMEM((8, slots, rows, LANES), jnp.float32),
            pltpu.VMEM((slots, rows, LANES), jnp.int32),
            pltpu.VMEM((6, rows, LANES), jnp.float32),
            pltpu.VMEM((rows, LANES), jnp.int32),
            pltpu.VMEM((2, -(-5 // cells_ra), rows, LANES), jnp.float32),
            pltpu.VMEM((2, rows, LANES), jnp.float32),
            pltpu.VMEM((2, -(-5 // cells_ra), rows, LANES), jnp.float32),
            pltpu.VMEM((6, rows, LANES), jnp.float32),
            pltpu.VMEM((45, rows, LANES), jnp.float32),
            pltpu.VMEM((9 * TERMS, rows, LANES), jnp.float32),
            pltpu.VMEM((TERMS, rows, LANES), jnp.float32),
            pltpu.VMEM((2, groups, rows, LANES), jnp.float32),
            pltpu.VMEM((2, groups, rows, LANES), jnp.float32),
            pltpu.VMEM((6, rows, LANES), jnp.float32),
            pltpu.VMEM((6, rows, LANES), jnp.float32),
            pltpu.VMEM((n_ra * n_dec, 1, LANES), jnp.float32),
            pltpu.VMEM((3, rows, LANES), jnp.int32),
            pltpu.SemaphoreType.DMA((4,)),
            pltpu.SemaphoreType.DMA((1,)),
            pltpu.SemaphoreType.DMA((1,)),
            pltpu.SemaphoreType.DMA((1,)),
            pltpu.SemaphoreType.DMA((1,)),
            pltpu.SemaphoreType.DMA((1,)),
            pltpu.SemaphoreType.REGULAR((2,)),
        ],
        compiler_params=pltpu.CompilerParams(collective_id=0, has_side_effects=True, vmem_limit_bytes=16*1024*1024),
    )(*[pltpu.with_memory_space_constraint(fold(x), pltpu.HBM) for x in (design, observed, weight, params, offsets, counts)])
    def finish(x_ref, c_ref, out_ref, s_ref):
        out_ref[...] = x_ref[...]
        s_ref[...] = c_ref[0:1, 0:1]
    new_params, chi = pl.pallas_call(
        finish,
        out_shape=(
            jax.ShapeDtypeStruct((5, rows, LANES), jnp.float32),
            jax.ShapeDtypeStruct((1, 1), jnp.float32),
        ),
        in_specs=[vmem, vmem],
        out_specs=(vmem, vmem),
        compiler_params=pltpu.CompilerParams(vmem_limit_bytes=1024*1024),
    )(new_params, chi)
    new_params = jnp.swapaxes(new_params.reshape(5, tiles, cells_ra, LANES), 1, 2)
    return new_params.reshape(params.shape), chi[0, 0]


def solution(mesh):
    return jax.shard_map(
        functools.partial(per_device, mesh.shape["ra"], mesh.shape["dec"]),
        mesh=mesh,
        in_specs=(
            P(None, None, "ra", "dec"),
            P(None, "ra", "dec"),
            P(None, "ra", "dec"),
            P(None, "ra", "dec"),
            P(None, "ra", "dec"),
            P("ra", "dec"),
        ),
        out_specs=(P(None, "ra", "dec"), P()),
        check_vma=False,
    )
```
